512 devices in a mesh: ctx: 256 (over z, y, x_hi, core), tp: 2 (over x_lo).
Axes of the slice: x: 4 (x_hi: 2, x_lo: 2; x = x_hi * 2 + x_lo), y: 8, z: 8, core: 2. Of those that a mesh axis runs over, the one named last changes fastest.
Arguments:
- queries: bfloat16 [16384, 16, 128], P('ctx', 'tp'), may hold values from -6 to 6
- incoming_lookup_vectors: bfloat16 [16384, 4, 128], P('ctx', 'tp'), may hold values from -6 to 6
- incoming_content_vectors: bfloat16 [16384, 4, 128], P('ctx', 'tp'), may hold values from -6 to 6
Outputs:
- attention: bfloat16 [16384, 16, 128], P(('ctx', 'tp'))
- key_cache: bfloat16 [16384, 4, 128], P('ctx', 'tp')
The draws below stay inside these ranges and needn't reach their ends.
All inputs are finite; a program needn't handle non-finite values.
Results may differ from the reference program's by a relative error of at most 0.0075.
Values may be sent and summed in bfloat16 or wider, within the bound.
A program may use at most 128 MiB of HBM per device.

```python
import math
import jax
import jax.numpy as jnp
from jax import lax

ASKING_HEAD_COUNT = 16
SHARED_HEAD_COUNT = 4
HEAD_WIDTH = 128
SEQUENCE_LENGTH = 16384


def levels(stream_key, extent, shards, low, top_value):
    factor_of, own = 1.0, jax.random.fold_in(stream_key, 6)
    for axis_at, shards_of in shards:
        steps = jnp.exp(jax.random.uniform(jax.random.fold_in(own, axis_at), (shards_of,), jnp.float32, low / len(shards), top_value / len(shards)))
        factor_of = factor_of * jnp.repeat(steps, extent[axis_at] // shards_of).reshape([-1 if axis == axis_at else 1 for axis in range(len(extent))])
    return factor_of


def normal_values(own_key, dims, scale, bound, cuts=(), kind=jnp.bfloat16):
    entries = jax.random.normal(own_key, dims, jnp.float32) * scale
    if len(cuts) > 0:
        entries = levels(own_key, dims, cuts, -0.22, 0.18) * entries
    return jnp.clip(entries, min=-bound, max=bound).astype(kind)


def setup_inputs(seed: int = 0) -> dict:
    streams_of = jax.random.split(jax.random.key(seed), 4)
    queries = normal_values(streams_of[0], (SEQUENCE_LENGTH, ASKING_HEAD_COUNT, HEAD_WIDTH), 1.0, 6.0, ((0, 256), (1, 2)))
    incoming_lookup_vectors = normal_values(streams_of[1], (SEQUENCE_LENGTH, SHARED_HEAD_COUNT, HEAD_WIDTH), 1.0, 6.0, ((0, 256), (1, 2)))
    incoming_content_vectors = normal_values(streams_of[2], (SEQUENCE_LENGTH, SHARED_HEAD_COUNT, HEAD_WIDTH), 1.0, 6.0, ((0, 256), (1, 2)))
    return dict(queries=queries, incoming_lookup_vectors=incoming_lookup_vectors, incoming_content_vectors=incoming_content_vectors)


rope_base = 500000.0

def rotate(tensor, positions):
    feature_width = tensor.shape[-1]
    half_width = feature_width // 2
    inverse_freq = rope_base ** (-(jnp.arange(half_width, dtype=jnp.float32) * 2.0 / feature_width))
    angles = positions.astype(jnp.float32)[:, None] * inverse_freq[None, :]
    cosine = jnp.cos(angles)[:, None, :]
    sine_part = jnp.sin(angles)[:, None, :]
    widened = tensor.astype(jnp.float32)
    front_half = widened[..., :half_width]
    second = widened[..., half_width:]
    return jnp.concatenate([front_half * cosine - second * sine_part, second * cosine + front_half * sine_part], axis=-1).astype(jnp.bfloat16)

def reference(queries, incoming_lookup_vectors, incoming_content_vectors):
    seq_len = queries.shape[0]
    positions = jnp.arange(seq_len, dtype=jnp.int32)
    key_cache = rotate(incoming_lookup_vectors, positions)
    spun_vectors = rotate(queries, positions)
    heads_per_share = ASKING_HEAD_COUNT // SHARED_HEAD_COUNT
    score_scale = 1.0 / math.sqrt(HEAD_WIDTH)
    piece_height = math.gcd(seq_len, 1024)
    number_of_pieces = seq_len // piece_height
    gathered_heads = spun_vectors.reshape(number_of_pieces, piece_height, SHARED_HEAD_COUNT, heads_per_share, HEAD_WIDTH).transpose(2, 0, 1, 3, 4)
    block_starts = jnp.arange(number_of_pieces, dtype=jnp.int32) * piece_height

    def attend_group(operands):
        q_group, key_head, value_head = operands
        key_wide = key_head.astype(jnp.float32)
        value_wide = value_head.astype(jnp.float32)

        def attend_block(block_operands):
            q_block, block_start = block_operands
            row_pos = block_start + jnp.arange(piece_height, dtype=jnp.int32)
            causal = row_pos[:, None] >= positions[None, :]
            scores = jnp.einsum('sgd,td->gst', q_block.astype(jnp.float32), key_wide) * score_scale
            scores = jnp.where(causal[None], scores, -jnp.inf)
            weights = jax.nn.softmax(scores, axis=-1)
            return jnp.einsum('gst,td->sgd', weights, value_wide)
        return lax.map(attend_block, (q_group, block_starts))
    result = lax.map(attend_group, (gathered_heads, key_cache.transpose(1, 0, 2), incoming_content_vectors.transpose(1, 0, 2)))
    attention = result.transpose(1, 2, 0, 3, 4).reshape(seq_len, ASKING_HEAD_COUNT, HEAD_WIDTH).astype(jnp.bfloat16)
    return (attention, key_cache)
```

```python
import functools
import math

import jax
import jax.numpy as jnp
import numpy as np
from jax import lax
from jax.experimental import pallas as pl
from jax.experimental.pallas import tpu as pltpu
from jax.sharding import PartitionSpec as P

rope_base = 500000.0
MESH = pl.DeviceIdType.MESH
ROW = 4
RING = 8
ORDER = (0, 1, 7, 2, 6, 3, 5, 4)
MAJOR = -1
FAR, NEAR = 4, 3
NEVER = -1e30


def angle_tables(blocks, rows, width):
    half = width // 2
    freq = rope_base ** (-(np.arange(half, dtype=np.float64) * 2.0 / width))
    freq = np.concatenate([freq, freq])[None, :]
    fine = np.arange(rows, dtype=np.float64)[:, None] * freq
    coarse = np.arange(blocks, dtype=np.float64)[:, None] * rows * freq
    fine_table = np.stack([np.cos(fine), np.sin(fine)]).astype(np.float32)
    coarse_table = np.stack([np.cos(coarse), np.sin(coarse)], 1).astype(np.float32)
    coarse_table = np.broadcast_to(coarse_table[:, :, None, :], (blocks, 2, 8, width))
    return fine_table, np.ascontiguousarray(coarse_table)


def kernel(
    heads,
    kv_heads,
    q_hbm,
    k_hbm,
    v_hbm,
    fine_hbm,
    coarse_hbm,
    att_hbm,
    cache_hbm,
    q_in,
    k_in,
    v_in,
    fine,
    coarse,
    wide_kv,
    wide_q,
    kv_own,
    kv,
    q_send,
    q_all,
    run_max,
    run_acc,
    out_send,
    out_recv,
    stat_send,
    stat_recv,
    wide_out,
    att_vmem,
    cache_vmem,
    load_sem,
    store_sem,
    twin_send,
    twin_recv,
    first_send,
    first_recv,
    unit_send,
    unit_recv,
    q_send_sem,
    q_recv_sem,
    out_send_sem,
    out_recv_sem,
    stat_send_sem,
    stat_recv_sem,
):
    rows = k_in.shape[0] // kv_heads
    width = k_in.shape[1]
    half_width = width // 2
    group = heads // kv_heads
    keep = rows // 2
    span = 2 * rows
    piece = group * keep
    keys = RING * span
    me = lax.axis_index("ctx")
    part = lax.axis_index("tp")
    core = me % 2
    x_hi = (me // 2) % 2
    y_at = (me // ROW) % RING
    z_at = me // (ROW * RING)
    along_y = 1 - core
    a = along_y * y_at + core * z_at
    u = along_y * z_at + core * y_at
    first_stride = along_y * ROW + core * ROW * RING
    second_stride = along_y * ROW * RING + core * ROW
    row_base = me - me % ROW
    twin = me + 1 - 2 * core
    place = (me % ROW) * 2 + part

    def first_peer(f):
        return me + (f - a) * first_stride

    def second_peer(w):
        return me + (w - u) * second_stride

    def up_by(value, d):
        return lax.rem(value + d + RING, RING)

    def row_peer(d):
        return {"ctx": row_base + d // 2, "tp": d % 2}

    loads = [
        pltpu.make_async_copy(k_hbm, k_in, load_sem.at[0]),
        pltpu.make_async_copy(v_hbm, v_in, load_sem.at[1]),
        pltpu.make_async_copy(fine_hbm, fine, load_sem.at[2]),
        pltpu.make_async_copy(coarse_hbm.at[me], coarse, load_sem.at[3]),
        pltpu.make_async_copy(q_hbm, q_in, load_sem.at[4]),
    ]
    barrier = pltpu.get_barrier_semaphore()
    for d in range(1, RING):
        to = first_peer(up_by(a, d))
        pl.semaphore_signal(barrier, inc=1, device_id={"ctx": to}, device_id_type=MESH)
    for d in (1, -1):
        to = second_peer(up_by(u, d))
        pl.semaphore_signal(barrier, inc=1, device_id={"ctx": to}, device_id_type=MESH)
    for i in range(1, 8):
        to = row_peer(lax.rem(place + i, 8))
        pl.semaphore_signal(barrier, inc=1, device_id=to, device_id_type=MESH)

    for load in loads:
        load.start()

    loads[2].wait()
    loads[3].wait()
    cos_c = coarse[0, 0:1, :]
    sin_c = coarse[1, 0:1, :]
    cosine = cos_c * fine[0] - sin_c * fine[1]
    sine = sin_c * fine[0] + cos_c * fine[1]
    lane = lax.broadcasted_iota(jnp.int32, (rows, width), 1)
    sine = jnp.where(lane < half_width, -sine, sine)

    def turn(x):
        return x * cosine + pltpu.roll(x, half_width, 1) * sine

    loads[0].wait()
    loads[1].wait()
    wide_kv[0] = k_in[...].astype(jnp.float32)
    wide_kv[1] = v_in[...].astype(jnp.float32)
    for j in range(kv_heads):
        take = pl.ds(j, rows, stride=kv_heads)
        key_rot = turn(wide_kv[0, take, :])
        wide_kv[0, take, :] = key_rot
        kv_own[j, 0] = key_rot.astype(jnp.bfloat16)
        kv_own[j, 1] = wide_kv[1, take, :].astype(jnp.bfloat16)
    kv[u, a, core] = kv_own[core]
    cache_vmem[...] = wide_kv[0].astype(jnp.bfloat16)
    cache_store = pltpu.make_async_copy(cache_vmem, cache_hbm, store_sem.at[0])
    cache_store.start()

    pl.semaphore_wait(barrier, (RING - 1) + 2 + 7)

    def twin_copy(unit, f, half):
        return pltpu.make_async_remote_copy(
            src_ref=kv_own.at[1 - core],
            dst_ref=kv.at[unit, f, half],
            send_sem=twin_send,
            recv_sem=twin_recv,
            device_id={"ctx": twin},
            device_id_type=MESH,
        )

    twin_copy(a, u, core).start()

    loads[4].wait()
    wide_q[...] = q_in[...].astype(jnp.float32)
    for h in range(heads):
        turned = turn(wide_q[pl.ds(h, rows, stride=heads), :]).astype(jnp.bfloat16)
        for half in range(2):
            q_send[h // group, half, h % group] = turned[half * keep : (half + 1) * keep]

    def first_copy(f, to, slot):
        return pltpu.make_async_remote_copy(
            src_ref=kv.at[u, f],
            dst_ref=kv.at[u, f],
            send_sem=first_send.at[slot],
            recv_sem=first_recv.at[f],
            device_id={"ctx": to},
            device_id_type=MESH,
        )

    def unit_copy(unit, f, to, slot):
        return pltpu.make_async_remote_copy(
            src_ref=kv.at[unit, f],
            dst_ref=kv.at[unit, f],
            send_sem=unit_send.at[slot, f],
            recv_sem=unit_recv.at[unit, f],
            device_id={"ctx": to},
            device_id_type=MESH,
        )

    major_to = second_peer(up_by(u, MAJOR))
    minor_to = second_peer(up_by(u, -MAJOR))

    twin_copy(u, a, 1 - core).wait_recv()
    for i in range(1, RING):
        first_copy(a, first_peer(up_by(a, ORDER[i])), i).start()
    unit_copy(u, a, major_to, 0).start()
    unit_copy(u, a, minor_to, 1).start()

    own_slot = me % ROW

    def q_copy(slot, to_slot, index):
        return pltpu.make_async_remote_copy(
            src_ref=q_send.at[to_slot % 2],
            dst_ref=q_all.at[slot],
            send_sem=q_send_sem.at[index],
            recv_sem=q_recv_sem.at[slot],
            device_id={"ctx": row_base + to_slot},
            device_id_type=MESH,
        )

    for i in range(1, ROW):
        q_copy(own_slot, lax.rem(own_slot + i, ROW), i).start()
    q_all[own_slot] = q_send[core]
    run_max[...] = jnp.full(run_max.shape, NEVER, jnp.float32)
    run_acc[...] = jnp.zeros(run_acc.shape, jnp.float32)

    for i in range(1, RING):
        f = up_by(a, ORDER[i])
        first_copy(f, me, i).wait_recv()
        unit_copy(u, f, major_to, 0).start()
        unit_copy(u, f, minor_to, 1).start()
    for i in range(1, ROW):
        slot = lax.rem(own_slot + i, ROW)
        q_copy(slot, own_slot, i).wait_recv()

    factor = math.log2(math.e) / math.sqrt(width)
    unit_step = along_y * (span * 2 * RING) + core * span * 2
    block_step = along_y * span * 2 + core * (span * 2 * RING)
    row_start = (z_at * RING + y_at) * span * 2

    def absorb(unit):
        key_block = kv[unit, :, :, 0].reshape(keys, width)
        value_block = kv[unit, :, :, 1].reshape(keys, width)
        extended = jnp.concatenate([value_block, jnp.ones_like(value_block)], axis=1)

        def chunk(r, carry):
            q = q_all[r].reshape(2 * piece, width)
            scores = factor * lax.dot_general(
                q, key_block, (((1,), (1,)), ((), ())), preferred_element_type=jnp.float32
            )
            at = lax.broadcasted_iota(jnp.int32, (2 * piece, 1), 0)
            q_at = row_start + (2 * r + at // piece) * keep + at % keep
            col = lax.broadcasted_iota(jnp.int32, (1, keys), 1)
            k_at = unit * unit_step + (col // span) * block_step + x_hi * span + col % span
            scores = jnp.where(k_at <= q_at, scores, NEVER)
            take = pl.ds(pl.multiple_of(r * 2 * piece, 2 * piece), 2 * piece)
            old = run_max[take, 0:1]
            top = jnp.maximum(old, jnp.max(scores, axis=1, keepdims=True))
            weights = jnp.exp2(scores - top).astype(jnp.bfloat16)
            total = jnp.dot(weights, extended, preferred_element_type=jnp.float32)
            run_acc[take, :] = total + jnp.exp2(old - top) * run_acc[take, :]
            run_max[take, :] = jnp.broadcast_to(top, (2 * piece, width))
            return carry

        lax.fori_loop(0, ROW, chunk, 0)

    def step_of(step):
        d = (step + 1) // 2
        odd = step % 2
        unit = up_by(u, (1 - 2 * odd) * MAJOR * d)
        far = up_by(u, (2 * odd - 1) * MAJOR)
        return d, odd, unit, far

    def advance(step, carry):
        d, odd, unit, far = step_of(step)
        to = second_peer(far)

        @pl.when(step > 0)
        def _():
            for i in range(RING):
                f = up_by(a, ORDER[i])
                unit_copy(unit, f, me, 0).wait_recv()

                @pl.when(d < NEAR + odd * (FAR - NEAR))
                def _():
                    unit_copy(unit, f, to, step + 1).start()

        @pl.when((unit <= u) | ((core == 1) & (z_at > 0)))
        def _():
            absorb(unit)

        return carry

    lax.fori_loop(0, RING, advance, 0)

    def out_copy(slot, d, index):
        return pltpu.make_async_remote_copy(
            src_ref=out_send.at[d],
            dst_ref=out_recv.at[slot],
            send_sem=out_send_sem.at[index],
            recv_sem=out_recv_sem.at[slot],
            device_id=row_peer(d),
            device_id_type=MESH,
        )

    def stat_copy(slot, d, index):
        return pltpu.make_async_remote_copy(
            src_ref=stat_send.at[d],
            dst_ref=stat_recv.at[slot],
            send_sem=stat_send_sem.at[index],
            recv_sem=stat_recv_sem.at[slot],
            device_id=row_peer(d),
            device_id_type=MESH,
        )

    def finish(d):
        take = pl.ds(pl.multiple_of(d * piece, piece), piece)
        weight = run_acc[take, width:]
        stat = run_max[take, :] + math.log2(math.e) * jnp.log(weight)
        return (run_acc[take, :width] / weight).astype(jnp.bfloat16), stat.T[0:8]

    out_order = (4, 5, 6, 7, 2, 3, 1)
    for i in out_order:
        d = lax.rem(place + i, 8)
        out_send[d], stat_send[d] = finish(d)
        out_copy(place, d, i).start()
        stat_copy(place, d, i).start()
    out_recv[place], stat_recv[place] = finish(place)

    for i in out_order:
        slot = lax.rem(place + i, 8)
        out_copy(slot, place, i).wait_recv()
        stat_copy(slot, place, i).wait_recv()

    for core_from in range(2):
        for tp_from in range(2):
            low = core_from * 2 + tp_from
            wide_stat = [
                jnp.broadcast_to(stat_recv[s, 0:1, :], (piece, width)).T for s in (low, low + 4)
            ]
            gap = wide_stat[1] - wide_stat[0]
            merged = out_recv[low].astype(jnp.float32) / (1.0 + jnp.exp2(gap))
            merged = merged + out_recv[low + 4].astype(jnp.float32) / (1.0 + jnp.exp2(-gap))
            for g in range(group):
                head = tp_from * heads + core_from * group + g
                wide_out[pl.ds(head, keep, stride=2 * heads), :] = merged[g * keep : (g + 1) * keep]
    att_vmem[...] = wide_out[...].astype(jnp.bfloat16)
    att_store = pltpu.make_async_copy(att_vmem, att_hbm, store_sem.at[1])
    att_store.start()

    twin_copy(a, u, core).wait_send()
    for i in range(1, RING):
        first_copy(a, me, i).wait_send()
    for i in range(1, ROW):
        q_copy(own_slot, lax.rem(own_slot + i, ROW), i).wait_send()
    for i in out_order:
        out_copy(place, lax.rem(place + i, 8), i).wait_send()
        stat_copy(place, lax.rem(place + i, 8), i).wait_send()

    def drain(slot, carry):
        for f in range(RING):
            unit_copy(u, f, me, slot).wait_send()
        return carry

    lax.fori_loop(0, RING - 1, drain, 0)
    cache_store.wait()
    att_store.wait()


def build(ctx_size, queries, keys_in, values_in):
    rows, heads, width = queries.shape
    kv_heads = keys_in.shape[1]
    group = heads // kv_heads
    keep = rows // 2
    piece = group * keep
    fine, coarse = angle_tables(ctx_size, rows, width)
    f32, bf16 = jnp.float32, jnp.bfloat16

    hbm = pl.BlockSpec(memory_space=pl.ANY)
    dma = pltpu.SemaphoreType.DMA
    att, cache = pl.pallas_call(
        functools.partial(kernel, heads, kv_heads),
        out_shape=(
            jax.ShapeDtypeStruct((2 * heads * keep, width), bf16),
            jax.ShapeDtypeStruct((rows * kv_heads, width), bf16),
        ),
        in_specs=[hbm] * 5,
        out_specs=(hbm, hbm),
        scratch_shapes=[
            pltpu.VMEM((rows * heads, width), bf16),
            pltpu.VMEM((rows * kv_heads, width), bf16),
            pltpu.VMEM((rows * kv_heads, width), bf16),
            pltpu.VMEM((2, rows, width), f32),
            pltpu.VMEM((2, 8, width), f32),
            pltpu.VMEM((2, rows * kv_heads, width), f32),
            pltpu.VMEM((rows * heads, width), f32),
            pltpu.VMEM((kv_heads, 2, rows, width), bf16),
            pltpu.VMEM((RING, RING, 2, 2, rows, width), bf16),
            pltpu.VMEM((2, 2, group, keep, width), bf16),
            pltpu.VMEM((ROW, 2, group, keep, width), bf16),
            pltpu.VMEM((8 * piece, width), f32),
            pltpu.VMEM((8 * piece, 2 * width), f32),
            pltpu.VMEM((8, piece, width), bf16),
            pltpu.VMEM((8, piece, width), bf16),
            pltpu.VMEM((8, 8, piece), f32),
            pltpu.VMEM((8, 8, piece), f32),
            pltpu.VMEM((2 * heads * keep, width), f32),
            pltpu.VMEM((2 * heads * keep, width), bf16),
            pltpu.VMEM((rows * kv_heads, width), bf16),
            dma((5,)),
            dma((2,)),
            dma,
            dma,
            dma((RING,)),
            dma((RING,)),
            dma((RING - 1, RING)),
            dma((RING, RING)),
            dma((ROW,)),
            dma((ROW,)),
            dma((8,)),
            dma((8,)),
            dma((8,)),
            dma((8,)),
        ],
        compiler_params=pltpu.CompilerParams(collective_id=0, has_side_effects=True),
    )(
        queries.reshape(rows * heads, width),
        keys_in.reshape(rows * kv_heads, width),
        values_in.reshape(rows * kv_heads, width),
        jnp.asarray(fine),
        jnp.asarray(coarse),
    )
    return att.reshape(keep, 2 * heads, width), cache.reshape(rows, kv_heads, width)


def solution(mesh):
    ctx_size = mesh.shape["ctx"]

    def per_device(queries, incoming_lookup_vectors, incoming_content_vectors):
        return build(ctx_size, queries, incoming_lookup_vectors, incoming_content_vectors)

    return jax.shard_map(
        per_device,
        mesh=mesh,
        in_specs=(P("ctx", "tp", None), P("ctx", "tp", None), P("ctx", "tp", None)),
        out_specs=(P(("ctx", "tp"), None, None), P("ctx", "tp", None)),
        check_vma=False,
    )
```

```python
import functools
import math

import jax
import jax.numpy as jnp
import numpy as np
from jax import lax
from jax.experimental import pallas as pl
from jax.experimental.pallas import tpu as pltpu
from jax.sharding import PartitionSpec as P

rope_base = 500000.0
MESH = pl.DeviceIdType.MESH
ROW = 4
RING = 8
ORDER = (0, 1, 7, 2, 6, 3, 5, 4)
MAJOR = -1
FAR, NEAR = 4, 3
NEVER = -1e30
CH, NB = 256, 2


def angle_tables(blocks, rows, width):
    half = width // 2
    freq = rope_base ** (-(np.arange(half, dtype=np.float64) * 2.0 / width))
    freq = np.concatenate([freq, freq])[None, :]
    fine = np.arange(rows, dtype=np.float64)[:, None] * freq
    coarse = np.arange(blocks, dtype=np.float64)[:, None] * rows * freq
    fine_table = np.stack([np.cos(fine), np.sin(fine)]).astype(np.float32)
    coarse_table = np.stack([np.cos(coarse), np.sin(coarse)], 1).astype(np.float32)
    coarse_table = np.broadcast_to(coarse_table[:, :, None, :], (blocks, 2, 8, width))
    return fine_table, np.ascontiguousarray(coarse_table)


def kernel(
    heads,
    kv_heads,
    q_hbm,
    k_hbm,
    v_hbm,
    fine_hbm,
    coarse_hbm,
    att_hbm,
    cache_hbm,
    q_in,
    k_in,
    v_in,
    fine,
    coarse,
    wide_kv,
    wide_q,
    kv_own,
    kv,
    q_send,
    q_all,
    run_max,
    run_acc,
    score_buf,
    out_send,
    out_recv,
    stat_send,
    stat_recv,
    wide_out,
    att_vmem,
    cache_vmem,
    load_sem,
    store_sem,
    twin_send,
    twin_recv,
    first_send,
    first_recv,
    unit_send,
    unit_recv,
    q_send_sem,
    q_recv_sem,
    out_send_sem,
    out_recv_sem,
    stat_send_sem,
    stat_recv_sem,
):
    rows = k_in.shape[0] // kv_heads
    width = k_in.shape[1]
    half_width = width // 2
    group = heads // kv_heads
    keep = rows // 2
    span = 2 * rows
    piece = group * keep
    keys = RING * span
    me = lax.axis_index("ctx")
    part = lax.axis_index("tp")
    core = me % 2
    x_hi = (me // 2) % 2
    y_at = (me // ROW) % RING
    z_at = me // (ROW * RING)
    along_y = 1 - core
    a = along_y * y_at + core * z_at
    u = along_y * z_at + core * y_at
    first_stride = along_y * ROW + core * ROW * RING
    second_stride = along_y * ROW * RING + core * ROW
    row_base = me - me % ROW
    twin = me + 1 - 2 * core
    place = (me % ROW) * 2 + part

    def first_peer(f):
        return me + (f - a) * first_stride

    def second_peer(w):
        return me + (w - u) * second_stride

    def up_by(value, d):
        return lax.rem(value + d + RING, RING)

    def row_peer(d):
        return {"ctx": row_base + d // 2, "tp": d % 2}

    loads = [
        pltpu.make_async_copy(k_hbm, k_in, load_sem.at[0]),
        pltpu.make_async_copy(v_hbm, v_in, load_sem.at[1]),
        pltpu.make_async_copy(fine_hbm, fine, load_sem.at[2]),
        pltpu.make_async_copy(coarse_hbm.at[me], coarse, load_sem.at[3]),
        pltpu.make_async_copy(q_hbm, q_in, load_sem.at[4]),
    ]
    barrier = pltpu.get_barrier_semaphore()
    for d in range(1, RING):
        to = first_peer(up_by(a, d))
        pl.semaphore_signal(barrier, inc=1, device_id={"ctx": to}, device_id_type=MESH)
    for d in (1, -1):
        to = second_peer(up_by(u, d))
        pl.semaphore_signal(barrier, inc=1, device_id={"ctx": to}, device_id_type=MESH)
    for i in range(1, 8):
        to = row_peer(lax.rem(place + i, 8))
        pl.semaphore_signal(barrier, inc=1, device_id=to, device_id_type=MESH)

    for load in loads:
        load.start()

    loads[2].wait()
    loads[3].wait()
    cos_c = coarse[0, 0:1, :]
    sin_c = coarse[1, 0:1, :]
    cosine = cos_c * fine[0] - sin_c * fine[1]
    sine = sin_c * fine[0] + cos_c * fine[1]
    lane = lax.broadcasted_iota(jnp.int32, (rows, width), 1)
    sine = jnp.where(lane < half_width, -sine, sine)

    def turn(x):
        return x * cosine + pltpu.roll(x, half_width, 1) * sine

    loads[0].wait()
    loads[1].wait()
    wide_kv[0] = k_in[...].astype(jnp.float32)
    wide_kv[1] = v_in[...].astype(jnp.float32)
    for j in range(kv_heads):
        take = pl.ds(j, rows, stride=kv_heads)
        key_rot = turn(wide_kv[0, take, :])
        wide_kv[0, take, :] = key_rot
        kv_own[j, 0] = key_rot.astype(jnp.bfloat16)
        kv_own[j, 1] = wide_kv[1, take, :].astype(jnp.bfloat16)
    kv[u, a, core] = kv_own[core]
    cache_vmem[...] = wide_kv[0].astype(jnp.bfloat16)
    cache_store = pltpu.make_async_copy(cache_vmem, cache_hbm, store_sem.at[0])
    cache_store.start()

    pl.semaphore_wait(barrier, (RING - 1) + 2 + 7)

    def twin_copy(unit, f, half):
        return pltpu.make_async_remote_copy(
            src_ref=kv_own.at[1 - core],
            dst_ref=kv.at[unit, f, half],
            send_sem=twin_send,
            recv_sem=twin_recv,
            device_id={"ctx": twin},
            device_id_type=MESH,
        )

    twin_copy(a, u, core).start()

    loads[4].wait()
    wide_q[...] = q_in[...].astype(jnp.float32)
    for h in range(heads):
        turned = turn(wide_q[pl.ds(h, rows, stride=heads), :]).astype(jnp.bfloat16)
        for half in range(2):
            q_send[h // group, half, h % group] = turned[half * keep : (half + 1) * keep]

    def first_copy(f, to, slot):
        return pltpu.make_async_remote_copy(
            src_ref=kv.at[u, f],
            dst_ref=kv.at[u, f],
            send_sem=first_send.at[slot],
            recv_sem=first_recv.at[f],
            device_id={"ctx": to},
            device_id_type=MESH,
        )

    def unit_copy(unit, f, to, slot):
        return pltpu.make_async_remote_copy(
            src_ref=kv.at[unit, f],
            dst_ref=kv.at[unit, f],
            send_sem=unit_send.at[slot, f],
            recv_sem=unit_recv.at[unit, f],
            device_id={"ctx": to},
            device_id_type=MESH,
        )

    major_to = second_peer(up_by(u, MAJOR))
    minor_to = second_peer(up_by(u, -MAJOR))

    twin_copy(u, a, 1 - core).wait_recv()
    for i in range(1, RING):
        first_copy(a, first_peer(up_by(a, ORDER[i])), i).start()
    unit_copy(u, a, major_to, 0).start()
    unit_copy(u, a, minor_to, 1).start()

    own_slot = me % ROW

    def q_copy(slot, to_slot, index):
        return pltpu.make_async_remote_copy(
            src_ref=q_send.at[to_slot % 2],
            dst_ref=q_all.at[slot],
            send_sem=q_send_sem.at[index],
            recv_sem=q_recv_sem.at[slot],
            device_id={"ctx": row_base + to_slot},
            device_id_type=MESH,
        )

    for i in range(1, ROW):
        q_copy(own_slot, lax.rem(own_slot + i, ROW), i).start()
    q_all[own_slot] = q_send[core]
    run_max[...] = jnp.full(run_max.shape, NEVER, jnp.float32)
    run_acc[...] = jnp.zeros(run_acc.shape, jnp.float32)

    for i in range(1, RING):
        f = up_by(a, ORDER[i])
        first_copy(f, me, i).wait_recv()
        unit_copy(u, f, major_to, 0).start()
        unit_copy(u, f, minor_to, 1).start()
    for i in range(1, ROW):
        slot = lax.rem(own_slot + i, ROW)
        q_copy(slot, own_slot, i).wait_recv()

    factor = math.log2(math.e) / math.sqrt(width)
    unit_step = along_y * (span * 2 * RING) + core * span * 2
    block_step = along_y * span * 2 + core * (span * 2 * RING)
    row_start = (z_at * RING + y_at) * span * 2

    def absorb(unit):
        key_block = kv[unit, :, :, 0].reshape(keys, width)
        value_block = kv[unit, :, :, 1].reshape(keys, width)
        extended = jnp.concatenate([value_block, jnp.ones_like(value_block)], axis=1)
        col = lax.broadcasted_iota(jnp.int32, (1, keys), 1)
        k_at = unit * unit_step + (col // span) * block_step + x_hi * span + col % span - row_start
        at = lax.broadcasted_iota(jnp.int32, (CH, 1), 0)

        def score(r):
            q = q_all[...].reshape(8 * piece, width)[r * CH : (r + 1) * CH]
            scores = factor * lax.dot_general(
                q, key_block, (((1,), (1,)), ((), ())), preferred_element_type=jnp.float32
            )
            q_at = ((r * CH + at) // piece) * keep + at % keep
            score_buf[r % NB] = jnp.where(k_at <= q_at, scores, NEVER)

        def weigh(r):
            take = slice(r * CH, (r + 1) * CH)
            old = run_max[take, 0:1]
            top = jnp.maximum(old, jnp.max(score_buf[r % NB], axis=1, keepdims=True))
            weights = jnp.exp2(score_buf[r % NB] - top).astype(jnp.bfloat16)
            total = jnp.dot(weights, extended, preferred_element_type=jnp.float32)
            run_acc[take, :] = total + jnp.exp2(old - top) * run_acc[take, :]
            run_max[take, :] = jnp.broadcast_to(top, (CH, width))

        chunks = 8 * piece // CH
        score(0)
        for r in range(chunks):
            if r + 1 < chunks:
                score(r + 1)
            weigh(r)

    def step_of(step):
        d = (step + 1) // 2
        odd = step % 2
        unit = up_by(u, (1 - 2 * odd) * MAJOR * d)
        far = up_by(u, (2 * odd - 1) * MAJOR)
        return d, odd, unit, far

    def advance(step, carry):
        d, odd, unit, far = step_of(step)
        to = second_peer(far)

        @pl.when(step > 0)
        def _():
            for i in range(RING):
                f = up_by(a, ORDER[i])
                unit_copy(unit, f, me, 0).wait_recv()

                @pl.when(d < NEAR + odd * (FAR - NEAR))
                def _():
                    unit_copy(unit, f, to, step + 1).start()

        @pl.when((unit <= u) | ((core == 1) & (z_at > 0)))
        def _():
            absorb(unit)

        return carry

    lax.fori_loop(0, RING, advance, 0)

    def out_copy(slot, d, index):
        return pltpu.make_async_remote_copy(
            src_ref=out_send.at[d],
            dst_ref=out_recv.at[slot],
            send_sem=out_send_sem.at[index],
            recv_sem=out_recv_sem.at[slot],
            device_id=row_peer(d),
            device_id_type=MESH,
        )

    def stat_copy(slot, d, index):
        return pltpu.make_async_remote_copy(
            src_ref=stat_send.at[d],
            dst_ref=stat_recv.at[slot],
            send_sem=stat_send_sem.at[index],
            recv_sem=stat_recv_sem.at[slot],
            device_id=row_peer(d),
            device_id_type=MESH,
        )

    def finish(d):
        take = pl.ds(pl.multiple_of(d * piece, piece), piece)
        weight = run_acc[take, width:]
        stat = run_max[take, :] + math.log2(math.e) * jnp.log(weight)
        return (run_acc[take, :width] / weight).astype(jnp.bfloat16), stat.T[0:8]

    out_order = (4, 5, 6, 7, 2, 3, 1)
    for i in out_order:
        d = lax.rem(place + i, 8)
        out_send[d], stat_send[d] = finish(d)
        out_copy(place, d, i).start()
        stat_copy(place, d, i).start()
    out_recv[place], stat_recv[place] = finish(place)

    for i in out_order:
        slot = lax.rem(place + i, 8)
        out_copy(slot, place, i).wait_recv()
        stat_copy(slot, place, i).wait_recv()

    for core_from in range(2):
        for tp_from in range(2):
            low = core_from * 2 + tp_from
            wide_stat = [
                jnp.broadcast_to(stat_recv[s, 0:1, :], (piece, width)).T for s in (low, low + 4)
            ]
            gap = wide_stat[1] - wide_stat[0]
            merged = out_recv[low].astype(jnp.float32) / (1.0 + jnp.exp2(gap))
            merged = merged + out_recv[low + 4].astype(jnp.float32) / (1.0 + jnp.exp2(-gap))
            for g in range(group):
                head = tp_from * heads + core_from * group + g
                wide_out[pl.ds(head, keep, stride=2 * heads), :] = merged[g * keep : (g + 1) * keep]
    att_vmem[...] = wide_out[...].astype(jnp.bfloat16)
    att_store = pltpu.make_async_copy(att_vmem, att_hbm, store_sem.at[1])
    att_store.start()

    twin_copy(a, u, core).wait_send()
    for i in range(1, RING):
        first_copy(a, me, i).wait_send()
    for i in range(1, ROW):
        q_copy(own_slot, lax.rem(own_slot + i, ROW), i).wait_send()
    for i in out_order:
        out_copy(place, lax.rem(place + i, 8), i).wait_send()
        stat_copy(place, lax.rem(place + i, 8), i).wait_send()

    def drain(slot, carry):
        for f in range(RING):
            unit_copy(u, f, me, slot).wait_send()
        return carry

    lax.fori_loop(0, RING - 1, drain, 0)
    cache_store.wait()
    att_store.wait()


def build(ctx_size, queries, keys_in, values_in):
    rows, heads, width = queries.shape
    kv_heads = keys_in.shape[1]
    group = heads // kv_heads
    keep = rows // 2
    piece = group * keep
    fine, coarse = angle_tables(ctx_size, rows, width)
    f32, bf16 = jnp.float32, jnp.bfloat16

    hbm = pl.BlockSpec(memory_space=pl.ANY)
    dma = pltpu.SemaphoreType.DMA
    att, cache = pl.pallas_call(
        functools.partial(kernel, heads, kv_heads),
        out_shape=(
            jax.ShapeDtypeStruct((2 * heads * keep, width), bf16),
            jax.ShapeDtypeStruct((rows * kv_heads, width), bf16),
        ),
        in_specs=[hbm] * 5,
        out_specs=(hbm, hbm),
        scratch_shapes=[
            pltpu.VMEM((rows * heads, width), bf16),
            pltpu.VMEM((rows * kv_heads, width), bf16),
            pltpu.VMEM((rows * kv_heads, width), bf16),
            pltpu.VMEM((2, rows, width), f32),
            pltpu.VMEM((2, 8, width), f32),
            pltpu.VMEM((2, rows * kv_heads, width), f32),
            pltpu.VMEM((rows * heads, width), f32),
            pltpu.VMEM((kv_heads, 2, rows, width), bf16),
            pltpu.VMEM((RING, RING, 2, 2, rows, width), bf16),
            pltpu.VMEM((2, 2, group, keep, width), bf16),
            pltpu.VMEM((ROW, 2, group, keep, width), bf16),
            pltpu.VMEM((8 * piece, width), f32),
            pltpu.VMEM((8 * piece, 2 * width), f32),
            pltpu.VMEM((NB, CH, RING * 2 * rows), f32),
            pltpu.VMEM((8, piece, width), bf16),
            pltpu.VMEM((8, piece, width), bf16),
            pltpu.VMEM((8, 8, piece), f32),
            pltpu.VMEM((8, 8, piece), f32),
            pltpu.VMEM((2 * heads * keep, width), f32),
            pltpu.VMEM((2 * heads * keep, width), bf16),
            pltpu.VMEM((rows * kv_heads, width), bf16),
            dma((5,)),
            dma((2,)),
            dma,
            dma,
            dma((RING,)),
            dma((RING,)),
            dma((RING - 1, RING)),
            dma((RING, RING)),
            dma((ROW,)),
            dma((ROW,)),
            dma((8,)),
            dma((8,)),
            dma((8,)),
            dma((8,)),
        ],
        compiler_params=pltpu.CompilerParams(collective_id=0, has_side_effects=True),
    )(
        queries.reshape(rows * heads, width),
        keys_in.reshape(rows * kv_heads, width),
        values_in.reshape(rows * kv_heads, width),
        jnp.asarray(fine),
        jnp.asarray(coarse),
    )
    return att.reshape(keep, 2 * heads, width), cache.reshape(rows, kv_heads, width)


def solution(mesh):
    ctx_size = mesh.shape["ctx"]

    def per_device(queries, incoming_lookup_vectors, incoming_content_vectors):
        return build(ctx_size, queries, incoming_lookup_vectors, incoming_content_vectors)

    return jax.shard_map(
        per_device,
        mesh=mesh,
        in_specs=(P("ctx", "tp", None), P("ctx", "tp", None), P("ctx", "tp", None)),
        out_specs=(P(("ctx", "tp"), None, None), P("ctx", "tp", None)),
        check_vma=False,
    )
```

```python
import functools
import math

import jax
import jax.numpy as jnp
import numpy as np
from jax import lax
from jax.experimental import pallas as pl
from jax.experimental.pallas import tpu as pltpu
from jax.sharding import PartitionSpec as P

rope_base = 500000.0
MESH = pl.DeviceIdType.MESH
ROW = 4
RING = 8
ORDER = (0, 1, 7, 2, 6, 3, 5, 4)
MAJOR = -1
FAR, NEAR = 4, 3
NEVER = -1e30
CH, NB = 256, 2


def angle_tables(blocks, rows, width):
    half = width // 2
    freq = rope_base ** (-(np.arange(half, dtype=np.float64) * 2.0 / width))
    freq = np.concatenate([freq, freq])[None, :]
    fine = np.arange(rows, dtype=np.float64)[:, None] * freq
    coarse = np.arange(blocks, dtype=np.float64)[:, None] * rows * freq
    fine_table = np.stack([np.cos(fine), np.sin(fine)]).astype(np.float32)
    coarse_table = np.stack([np.cos(coarse), np.sin(coarse)], 1).astype(np.float32)
    coarse_table = np.broadcast_to(coarse_table[:, :, None, :], (blocks, 2, 8, width))
    return fine_table, np.ascontiguousarray(coarse_table)


def kernel(
    heads,
    kv_heads,
    q_hbm,
    k_hbm,
    v_hbm,
    fine_hbm,
    coarse_hbm,
    out_recv,
    stat_recv,
    cache_hbm,
    q_in,
    k_in,
    v_in,
    fine,
    coarse,
    wide_kv,
    wide_q,
    kv_own,
    kv,
    q_send,
    q_all,
    run_max,
    run_acc,
    score_buf,
    out_send,
    stat_send,
    cache_vmem,
    load_sem,
    store_sem,
    twin_send,
    twin_recv,
    first_send,
    first_recv,
    unit_send,
    unit_recv,
    q_send_sem,
    q_recv_sem,
    out_send_sem,
    out_recv_sem,
    stat_send_sem,
    stat_recv_sem,
):
    rows = k_in.shape[0] // kv_heads
    width = k_in.shape[1]
    half_width = width // 2
    group = heads // kv_heads
    keep = rows // 2
    span = 2 * rows
    piece = group * keep
    keys = RING * span
    me = lax.axis_index("ctx")
    part = lax.axis_index("tp")
    core = me % 2
    x_hi = (me // 2) % 2
    y_at = (me // ROW) % RING
    z_at = me // (ROW * RING)
    along_y = 1 - core
    a = along_y * y_at + core * z_at
    u = along_y * z_at + core * y_at
    first_stride = along_y * ROW + core * ROW * RING
    second_stride = along_y * ROW * RING + core * ROW
    row_base = me - me % ROW
    twin = me + 1 - 2 * core
    place = (me % ROW) * 2 + part

    def first_peer(f):
        return me + (f - a) * first_stride

    def second_peer(w):
        return me + (w - u) * second_stride

    def up_by(value, d):
        return lax.rem(value + d + RING, RING)

    def row_peer(d):
        return {"ctx": row_base + d // 2, "tp": d % 2}

    loads = [
        pltpu.make_async_copy(k_hbm, k_in, load_sem.at[0]),
        pltpu.make_async_copy(v_hbm, v_in, load_sem.at[1]),
        pltpu.make_async_copy(fine_hbm, fine, load_sem.at[2]),
        pltpu.make_async_copy(coarse_hbm.at[me], coarse, load_sem.at[3]),
        pltpu.make_async_copy(q_hbm, q_in, load_sem.at[4]),
    ]
    barrier = pltpu.get_barrier_semaphore()
    for d in range(1, RING):
        to = first_peer(up_by(a, d))
        pl.semaphore_signal(barrier, inc=1, device_id={"ctx": to}, device_id_type=MESH)
    for d in (1, -1):
        to = second_peer(up_by(u, d))
        pl.semaphore_signal(barrier, inc=1, device_id={"ctx": to}, device_id_type=MESH)
    for i in range(1, 8):
        to = row_peer(lax.rem(place + i, 8))
        pl.semaphore_signal(barrier, inc=1, device_id=to, device_id_type=MESH)

    for load in loads:
        load.start()

    loads[2].wait()
    loads[3].wait()
    cos_c = coarse[0, 0:1, :]
    sin_c = coarse[1, 0:1, :]
    cosine = cos_c * fine[0] - sin_c * fine[1]
    sine = sin_c * fine[0] + cos_c * fine[1]
    lane = lax.broadcasted_iota(jnp.int32, (rows, width), 1)
    sine = jnp.where(lane < half_width, -sine, sine)

    def turn(x):
        return x * cosine + pltpu.roll(x, half_width, 1) * sine

    loads[0].wait()
    loads[1].wait()
    wide_kv[0] = k_in[...].astype(jnp.float32)
    wide_kv[1] = v_in[...].astype(jnp.float32)
    for j in range(kv_heads):
        take = pl.ds(j, rows, stride=kv_heads)
        key_rot = turn(wide_kv[0, take, :])
        wide_kv[0, take, :] = key_rot
        kv_own[j, 0] = key_rot.astype(jnp.bfloat16)
        kv_own[j, 1] = wide_kv[1, take, :].astype(jnp.bfloat16)
    kv[u, a, core] = kv_own[core]
    cache_vmem[...] = wide_kv[0].astype(jnp.bfloat16)
    cache_store = pltpu.make_async_copy(cache_vmem, cache_hbm, store_sem.at[0])
    cache_store.start()
    pl.semaphore_wait(barrier, (RING - 1) + 2 + 7)

    def twin_copy(unit, f, half):
        return pltpu.make_async_remote_copy(
            src_ref=kv_own.at[1 - core],
            dst_ref=kv.at[unit, f, half],
            send_sem=twin_send,
            recv_sem=twin_recv,
            device_id={"ctx": twin},
            device_id_type=MESH,
        )

    def first_copy(f, half, to, slot):
        return pltpu.make_async_remote_copy(
            src_ref=kv.at[u, f, half],
            dst_ref=kv.at[u, f, half],
            send_sem=first_send.at[slot, half],
            recv_sem=first_recv.at[f, half],
            device_id={"ctx": to},
            device_id_type=MESH,
        )

    def unit_copy(unit, f, to, slot):
        return pltpu.make_async_remote_copy(
            src_ref=kv.at[unit, f],
            dst_ref=kv.at[unit, f],
            send_sem=unit_send.at[slot, f],
            recv_sem=unit_recv.at[unit, f],
            device_id={"ctx": to},
            device_id_type=MESH,
        )

    def q_copy(slot, to_slot, index):
        return pltpu.make_async_remote_copy(
            src_ref=q_send.at[to_slot % 2],
            dst_ref=q_all.at[slot],
            send_sem=q_send_sem.at[index],
            recv_sem=q_recv_sem.at[slot],
            device_id={"ctx": row_base + to_slot},
            device_id_type=MESH,
        )

    def climbs(unit):
        return (core == 1) | ((unit <= u) & (u < RING - 1))

    def wraps(unit):
        return (core == 1) | (unit < FAR)

    def spread(half, i_list):
        for i in i_list:
            to = up_by(a, ORDER[i])

            @pl.when((core == 0) | (to > a))
            def _():
                first_copy(a, half, first_peer(to), i).start()


    major_to = second_peer(up_by(u, MAJOR))
    minor_to = second_peer(up_by(u, -MAJOR))

    twin_copy(a, u, core).start()
    spread(core, (1, 2, 3, 4, 5, 6, 7))

    own_slot = me % ROW
    loads[4].wait()
    wide_q[...] = q_in[...].astype(jnp.float32)
    for h in range(heads):
        turned = turn(wide_q[pl.ds(h, rows, stride=heads), :]).astype(jnp.bfloat16)
        for half in range(2):
            q_send[h // group, half, h % group] = turned[half * keep : (half + 1) * keep]

    twin_copy(u, a, 1 - core).wait_recv()
    spread(1 - core, (1, 2, 3, 4, 5, 6, 7))
    pl.when(wraps(u))(lambda: unit_copy(u, a, major_to, 0).start())
    pl.when(climbs(u))(lambda: unit_copy(u, a, minor_to, 1).start())
    for i in range(1, ROW):
        q_copy(own_slot, lax.rem(own_slot + i, ROW), i).start()
    q_all[own_slot] = q_send[core]
    @pl.when(core == 1)
    def _():
        def clear(f, carry):
            kv[:, f] = jnp.zeros((RING, 2, 2, rows, width), jnp.bfloat16)
            return carry

        lax.fori_loop(a + 1, RING, clear, 0)

    run_max[...] = jnp.full(run_max.shape, NEVER, jnp.float32)
    run_acc[...] = jnp.zeros(run_acc.shape, jnp.float32)

    def next_hop(i):
        return first_peer(up_by(a, 1 if ORDER[i] > RING // 2 else -1))

    def pass_on(f, half, i, slot):
        first_copy(f, half, next_hop(i), slot).start()
        first_sends.append((half, slot))

    def early(i):
        f = up_by(a, ORDER[i])
        for k, to in ((0, major_to), (1, minor_to)):
            unit = up_by(u, (2 * k - 1) * MAJOR)
            unit_copy(unit, f, me, 0).wait_recv()
            unit_copy(unit, f, to, 2 + k).start()

    for i in range(1, RING):
        f = up_by(a, ORDER[i])

        @pl.when((core == 0) | (f < a))
        def _():
            for half in range(2):
                first_copy(f, half, me, i).wait_recv()

            @pl.when(wraps(u))
            def _():
                unit_copy(u, f, major_to, 0).start()

            @pl.when(climbs(u))
            def _():
                unit_copy(u, f, minor_to, 1).start()

    factor = math.log2(math.e) / math.sqrt(width)
    unit_step = along_y * (span * 2 * RING) + core * span * 2
    block_step = along_y * span * 2 + core * (span * 2 * RING)
    row_start = (z_at * RING + y_at) * span * 2

    def absorb(unit):
        key_block = kv[unit, :, :, 0].reshape(keys, width)
        value_block = kv[unit, :, :, 1].reshape(keys, width)
        extended = jnp.concatenate([value_block, jnp.ones_like(value_block)], axis=1)
        col = lax.broadcasted_iota(jnp.int32, (1, keys), 1)
        k_at = unit * unit_step + (col // span) * block_step + x_hi * span + col % span - row_start
        at = lax.broadcasted_iota(jnp.int32, (CH, 1), 0)

        def score(r):
            q = q_all[...].reshape(8 * piece, width)[r * CH : (r + 1) * CH]
            scores = factor * lax.dot_general(
                q, key_block, (((1,), (1,)), ((), ())), preferred_element_type=jnp.float32
            )
            q_at = ((r * CH + at) // piece) * keep + at % keep
            score_buf[r % NB] = jnp.where(k_at <= q_at, scores, NEVER)

        def weigh(r):
            take = slice(r * CH, (r + 1) * CH)
            old = run_max[take, 0:1]
            top = jnp.maximum(old, jnp.max(score_buf[r % NB], axis=1, keepdims=True))
            weights = jnp.exp2(score_buf[r % NB] - top).astype(jnp.bfloat16)
            total = jnp.dot(weights, extended, preferred_element_type=jnp.float32)
            run_acc[take, :] = total + jnp.exp2(old - top) * run_acc[take, :]
            run_max[take, :] = jnp.broadcast_to(top, (CH, width))

        chunks = 8 * piece // CH
        score(0)
        for r in range(chunks):
            if r + 1 < chunks:
                score(r + 1)
            weigh(r)

    def step_of(step):
        d = (step + 1) // 2
        odd = step % 2
        unit = up_by(u, (1 - 2 * odd) * MAJOR * d)
        far = up_by(u, (2 * odd - 1) * MAJOR)
        return d, odd, unit, far

    def advance(step, carry):
        d, odd, unit, far = step_of(step)
        to = second_peer(far)

        @pl.when(step > 0)
        def _():
            lands = (core == 1) | jnp.where(odd == 1, unit < FAR, unit < u)
            goes = (core == 1) | jnp.where(odd == 1, unit < FAR, (unit < u) & (u < RING - 1))
            goes = goes & (d < NEAR + odd * (FAR - NEAR))

            for i in range(RING):
                f = up_by(a, ORDER[i])

                @pl.when(lands & ((core == 0) | (f <= a)))
                def _():
                    unit_copy(unit, f, me, 0).wait_recv()

                    @pl.when(goes)
                    def _():
                        unit_copy(unit, f, to, step + 1).start()

        @pl.when(step == 0)
        def _():
            for i in range(1, ROW):
                slot = lax.rem(own_slot + i, ROW)
                q_copy(slot, own_slot, i).wait_recv()

        @pl.when((unit <= u) | ((core == 1) & (z_at > 0)))
        def _():
            absorb(unit)

        return carry

    lax.fori_loop(0, RING, advance, 0)

    def out_copy(slot, d, index):
        return pltpu.make_async_remote_copy(
            src_ref=out_send.at[d],
            dst_ref=out_recv.at[slot],
            send_sem=out_send_sem.at[index],
            recv_sem=out_recv_sem.at[slot],
            device_id=row_peer(d),
            device_id_type=MESH,
        )

    def stat_copy(slot, d, index):
        return pltpu.make_async_remote_copy(
            src_ref=stat_send.at[d],
            dst_ref=stat_recv.at[slot],
            send_sem=stat_send_sem.at[index],
            recv_sem=stat_recv_sem.at[slot],
            device_id=row_peer(d),
            device_id_type=MESH,
        )

    def finish(d):
        take = pl.ds(pl.multiple_of(d * piece, piece), piece)
        weight = run_acc[take, width:]
        stat = run_max[take, :] + math.log2(math.e) * jnp.log(weight)
        return (run_acc[take, :width] / weight).astype(jnp.bfloat16), stat.T[0:8]

    out_order = (4, 5, 6, 7, 2, 3, 1)
    for i in out_order:
        d = lax.rem(place + i, 8)
        out_send[d], stat_send[d] = finish(d)
        out_copy(place, d, i).start()
        stat_copy(place, d, i).start()
    out_send[place], stat_send[place] = finish(place)
    keeps = [
        pltpu.make_async_copy(out_send.at[place], out_recv.at[place], store_sem.at[1]),
        pltpu.make_async_copy(stat_send.at[place], stat_recv.at[place], store_sem.at[2]),
    ]
    for copy in keeps:
        copy.start()

    for i in out_order:
        slot = lax.rem(place + i, 8)
        out_copy(slot, place, i).wait_recv()
        stat_copy(slot, place, i).wait_recv()

    twin_copy(a, u, core).wait_send()
    for i in range(1, RING):

        @pl.when((core == 0) | (up_by(a, ORDER[i]) > a))
        def _():
            for half in range(2):
                first_copy(a, half, me, i).wait_send()

    for i in range(1, ROW):
        q_copy(own_slot, lax.rem(own_slot + i, ROW), i).wait_send()
    for i in out_order:
        out_copy(place, lax.rem(place + i, 8), i).wait_send()
        stat_copy(place, lax.rem(place + i, 8), i).wait_send()

    def drain(slot, carry):
        d = slot // 2
        odd = 1 - slot % 2
        unit = up_by(u, (1 - 2 * odd) * MAJOR * d)
        goes = (core == 1) | jnp.where(odd == 1, unit < FAR, (unit <= u) & (u < RING - 1))

        @pl.when(goes)
        def _():
            for f in range(RING):

                @pl.when((core == 0) | (f <= a))
                def _():
                    unit_copy(u, f, me, slot).wait_send()

        return carry

    lax.fori_loop(0, RING - 1, drain, 0)
    cache_store.wait()
    for copy in keeps:
        copy.wait()


def merge_kernel(heads, group, out_recv, stat_recv, cache_in, att, cache, wide_out):
    _, piece, width = out_recv.shape
    keep = piece // group
    cache[...] = cache_in[...]
    for core_from in range(2):
        for tp_from in range(2):
            low = core_from * 2 + tp_from
            wide_stat = [
                jnp.broadcast_to(stat_recv[s, 0:1, :], (piece, width)).T for s in (low, low + 4)
            ]
            gap = wide_stat[1] - wide_stat[0]
            merged = out_recv[low].astype(jnp.float32) / (1.0 + jnp.exp2(gap))
            merged = merged + out_recv[low + 4].astype(jnp.float32) / (1.0 + jnp.exp2(-gap))
            for g in range(group):
                head = tp_from * heads + core_from * group + g
                wide_out[pl.ds(head, keep, stride=2 * heads), :] = merged[g * keep : (g + 1) * keep]
    att[...] = wide_out[...].astype(jnp.bfloat16)


def build(ctx_size, queries, keys_in, values_in):
    rows, heads, width = queries.shape
    kv_heads = keys_in.shape[1]
    group = heads // kv_heads
    keep = rows // 2
    piece = group * keep
    fine, coarse = angle_tables(ctx_size, rows, width)
    f32, bf16 = jnp.float32, jnp.bfloat16

    hbm = pl.BlockSpec(memory_space=pl.ANY)
    dma = pltpu.SemaphoreType.DMA
    parts, stats, cache = pl.pallas_call(
        functools.partial(kernel, heads, kv_heads),
        out_shape=(
            jax.ShapeDtypeStruct((8, piece, width), bf16),
            jax.ShapeDtypeStruct((8, 8, piece), f32),
            jax.ShapeDtypeStruct((rows * kv_heads, width), bf16),
        ),
        in_specs=[hbm] * 5,
        out_specs=(hbm, hbm, hbm),
        scratch_shapes=[
            pltpu.VMEM((rows * heads, width), bf16),
            pltpu.VMEM((rows * kv_heads, width), bf16),
            pltpu.VMEM((rows * kv_heads, width), bf16),
            pltpu.VMEM((2, rows, width), f32),
            pltpu.VMEM((2, 8, width), f32),
            pltpu.VMEM((2, rows * kv_heads, width), f32),
            pltpu.VMEM((rows * heads, width), f32),
            pltpu.VMEM((kv_heads, 2, rows, width), bf16),
            pltpu.VMEM((RING, RING, 2, 2, rows, width), bf16),
            pltpu.VMEM((2, 2, group, keep, width), bf16),
            pltpu.VMEM((ROW, 2, group, keep, width), bf16),
            pltpu.VMEM((8 * piece, width), f32),
            pltpu.VMEM((8 * piece, 2 * width), f32),
            pltpu.VMEM((NB, CH, RING * 2 * rows), f32),
            pltpu.VMEM((8, piece, width), bf16),
            pltpu.VMEM((8, 8, piece), f32),
            pltpu.VMEM((rows * kv_heads, width), bf16),
            dma((5,)),
            dma((3,)),
            dma,
            dma,
            dma((2 * RING, 2)),
            dma((RING, 2)),
            dma((RING, RING)),
            dma((RING, RING)),
            dma((ROW,)),
            dma((ROW,)),
            dma((8,)),
            dma((8,)),
            dma((8,)),
            dma((8,)),
        ],
        compiler_params=pltpu.CompilerParams(collective_id=0, has_side_effects=True),
    )(
        queries.reshape(rows * heads, width),
        keys_in.reshape(rows * kv_heads, width),
        values_in.reshape(rows * kv_heads, width),
        jnp.asarray(fine),
        jnp.asarray(coarse),
    )
    vmem = pl.BlockSpec(memory_space=pltpu.VMEM)
    att, cache = pl.pallas_call(
        functools.partial(merge_kernel, heads, group),
        out_shape=(
            jax.ShapeDtypeStruct((2 * heads * keep, width), bf16),
            jax.ShapeDtypeStruct((rows * kv_heads, width), bf16),
        ),
        in_specs=[vmem] * 3,
        out_specs=(vmem, vmem),
        scratch_shapes=[pltpu.VMEM((2 * heads * keep, width), f32)],
    )(parts, stats, cache)
    return att.reshape(keep, 2 * heads, width), cache.reshape(rows, kv_heads, width)


def solution(mesh):
    ctx_size = mesh.shape["ctx"]

    def per_device(queries, incoming_lookup_vectors, incoming_content_vectors):
        return build(ctx_size, queries, incoming_lookup_vectors, incoming_content_vectors)

    return jax.shard_map(
        per_device,
        mesh=mesh,
        in_specs=(P("ctx", "tp", None), P("ctx", "tp", None), P("ctx", "tp", None)),
        out_specs=(P(("ctx", "tp"), None, None), P("ctx", "tp", None)),
        check_vma=False,
    )
```

```python
import functools
import math

import jax
import jax.numpy as jnp
import numpy as np
from jax import lax
from jax.experimental import pallas as pl
from jax.experimental.pallas import tpu as pltpu
from jax.sharding import PartitionSpec as P

rope_base = 500000.0
MESH = pl.DeviceIdType.MESH
ROW = 4
RING = 8
ORDER = (0, 1, 7, 2, 6, 3, 5, 4)
MAJOR = -1
FAR, NEAR = 4, 3
NEVER = -1e30
CH, NB = 256, 2


def angle_tables(blocks, rows, width):
    half = width // 2
    freq = rope_base ** (-(np.arange(half, dtype=np.float64) * 2.0 / width))
    freq = np.concatenate([freq, freq])[None, :]
    fine = np.arange(rows, dtype=np.float64)[:, None] * freq
    coarse = np.arange(blocks, dtype=np.float64)[:, None] * rows * freq
    fine_table = np.stack([np.cos(fine), np.sin(fine)]).astype(np.float32)
    coarse_table = np.stack([np.cos(coarse), np.sin(coarse)], 1).astype(np.float32)
    coarse_table = np.broadcast_to(coarse_table[:, :, None, :], (blocks, 2, 8, width))
    return fine_table, np.ascontiguousarray(coarse_table)


def kernel(
    heads,
    kv_heads,
    q_hbm,
    k_hbm,
    v_hbm,
    fine_hbm,
    coarse_hbm,
    out_recv,
    stat_recv,
    cache_hbm,
    q_in,
    k_in,
    v_in,
    fine,
    coarse,
    wide_kv,
    wide_q,
    kv_own,
    kv,
    q_send,
    q_all,
    run_max,
    run_acc,
    score_buf,
    out_send,
    stat_send,
    cache_vmem,
    load_sem,
    store_sem,
    twin_send,
    twin_recv,
    first_send,
    first_recv,
    unit_send,
    unit_recv,
    q_send_sem,
    q_recv_sem,
    out_send_sem,
    out_recv_sem,
    stat_send_sem,
    stat_recv_sem,
):
    rows = k_in.shape[0] // kv_heads
    width = k_in.shape[1]
    half_width = width // 2
    group = heads // kv_heads
    keep = rows // 2
    span = 2 * rows
    piece = group * keep
    keys = RING * span
    me = lax.axis_index("ctx")
    part = lax.axis_index("tp")
    core = me % 2
    x_hi = (me // 2) % 2
    y_at = (me // ROW) % RING
    z_at = me // (ROW * RING)
    along_y = 1 - core
    a = along_y * y_at + core * z_at
    u = along_y * z_at + core * y_at
    first_stride = along_y * ROW + core * ROW * RING
    second_stride = along_y * ROW * RING + core * ROW
    row_base = me - me % ROW
    twin = me + 1 - 2 * core
    place = (me % ROW) * 2 + part

    def first_peer(f):
        return me + (f - a) * first_stride

    def second_peer(w):
        return me + (w - u) * second_stride

    def up_by(value, d):
        return lax.rem(value + d + RING, RING)

    def row_peer(d):
        return {"ctx": row_base + d // 2, "tp": d % 2}

    loads = [
        pltpu.make_async_copy(k_hbm, k_in, load_sem.at[0]),
        pltpu.make_async_copy(v_hbm, v_in, load_sem.at[1]),
        pltpu.make_async_copy(fine_hbm, fine, load_sem.at[2]),
        pltpu.make_async_copy(coarse_hbm.at[me], coarse, load_sem.at[3]),
        pltpu.make_async_copy(q_hbm, q_in, load_sem.at[4]),
    ]
    barrier = pltpu.get_barrier_semaphore()
    for d in range(1, RING):
        to = first_peer(up_by(a, d))
        pl.semaphore_signal(barrier, inc=1, device_id={"ctx": to}, device_id_type=MESH)
    for d in (1, -1):
        to = second_peer(up_by(u, d))
        pl.semaphore_signal(barrier, inc=1, device_id={"ctx": to}, device_id_type=MESH)
    for i in range(1, 8):
        to = row_peer(lax.rem(place + i, 8))
        pl.semaphore_signal(barrier, inc=1, device_id=to, device_id_type=MESH)

    for load in loads:
        load.start()

    loads[2].wait()
    loads[3].wait()
    cos_c = coarse[0, 0:1, :]
    sin_c = coarse[1, 0:1, :]
    cosine = cos_c * fine[0] - sin_c * fine[1]
    sine = sin_c * fine[0] + cos_c * fine[1]
    lane = lax.broadcasted_iota(jnp.int32, (rows, width), 1)
    sine = jnp.where(lane < half_width, -sine, sine)

    def turn(x):
        return x * cosine + pltpu.roll(x, half_width, 1) * sine

    loads[0].wait()
    loads[1].wait()
    wide_kv[0] = k_in[...].astype(jnp.float32)
    wide_kv[1] = v_in[...].astype(jnp.float32)
    for j in range(kv_heads):
        take = pl.ds(j, rows, stride=kv_heads)
        key_rot = turn(wide_kv[0, take, :])
        wide_kv[0, take, :] = key_rot
        kv_own[j, 0] = key_rot.astype(jnp.bfloat16)
        kv_own[j, 1] = wide_kv[1, take, :].astype(jnp.bfloat16)
    kv[u, a, core] = kv_own[core]
    cache_vmem[...] = wide_kv[0].astype(jnp.bfloat16)
    cache_store = pltpu.make_async_copy(cache_vmem, cache_hbm, store_sem.at[0])
    cache_store.start()
    pl.semaphore_wait(barrier, (RING - 1) + 2 + 7)

    def twin_copy(unit, f, half):
        return pltpu.make_async_remote_copy(
            src_ref=kv_own.at[1 - core],
            dst_ref=kv.at[unit, f, half],
            send_sem=twin_send,
            recv_sem=twin_recv,
            device_id={"ctx": twin},
            device_id_type=MESH,
        )

    def first_copy(f, half, to, slot):
        return pltpu.make_async_remote_copy(
            src_ref=kv.at[u, f, half],
            dst_ref=kv.at[u, f, half],
            send_sem=first_send.at[slot, half],
            recv_sem=first_recv.at[f, half],
            device_id={"ctx": to},
            device_id_type=MESH,
        )

    def unit_copy(unit, f, to, slot):
        return pltpu.make_async_remote_copy(
            src_ref=kv.at[unit, f],
            dst_ref=kv.at[unit, f],
            send_sem=unit_send.at[slot, f],
            recv_sem=unit_recv.at[unit, f],
            device_id={"ctx": to},
            device_id_type=MESH,
        )

    def q_copy(slot, to_slot, index):
        return pltpu.make_async_remote_copy(
            src_ref=q_send.at[to_slot % 2],
            dst_ref=q_all.at[slot],
            send_sem=q_send_sem.at[index],
            recv_sem=q_recv_sem.at[slot],
            device_id={"ctx": row_base + to_slot},
            device_id_type=MESH,
        )

    spreads = (core == 0) & (u < RING - 1)

    def climbs(unit):
        return (core == 1) | ((unit <= u) & (u < RING - 1))

    def wraps(unit):
        return (core == 1) | (unit < FAR)

    def spread(half, i_list):
        for i in i_list:
            to = up_by(a, ORDER[i])

            @pl.when(spreads | (to > a))
            def _():
                first_copy(a, half, first_peer(to), i).start()


    major_to = second_peer(up_by(u, MAJOR))
    minor_to = second_peer(up_by(u, -MAJOR))

    twin_copy(a, u, core).start()
    spread(core, (1, 2, 3, 4, 5, 6, 7))

    own_slot = me % ROW
    loads[4].wait()
    wide_q[...] = q_in[...].astype(jnp.float32)
    for h in range(heads):
        turned = turn(wide_q[pl.ds(h, rows, stride=heads), :]).astype(jnp.bfloat16)
        for half in range(2):
            q_send[h // group, half, h % group] = turned[half * keep : (half + 1) * keep]

    twin_copy(u, a, 1 - core).wait_recv()
    spread(1 - core, (1, 2, 3, 4, 5, 6, 7))
    pl.when(wraps(u))(lambda: unit_copy(u, a, major_to, 0).start())
    pl.when(climbs(u))(lambda: unit_copy(u, a, minor_to, 1).start())
    for i in range(1, ROW):
        q_copy(own_slot, lax.rem(own_slot + i, ROW), i).start()
    q_all[own_slot] = q_send[core]
    @pl.when((core == 0) & (u == RING - 1))
    def _():
        def clear(f, carry):
            kv[u, f] = jnp.zeros((2, 2, rows, width), jnp.bfloat16)
            return carry

        lax.fori_loop(a + 1, RING, clear, 0)

    @pl.when(core == 1)
    def _():
        def clear(f, carry):
            kv[:, f] = jnp.zeros((RING, 2, 2, rows, width), jnp.bfloat16)
            return carry

        lax.fori_loop(a + 1, RING, clear, 0)

    run_max[...] = jnp.full(run_max.shape, NEVER, jnp.float32)
    run_acc[...] = jnp.zeros(run_acc.shape, jnp.float32)

    def next_hop(i):
        return first_peer(up_by(a, 1 if ORDER[i] > RING // 2 else -1))

    def pass_on(f, half, i, slot):
        first_copy(f, half, next_hop(i), slot).start()
        first_sends.append((half, slot))

    def early(i):
        f = up_by(a, ORDER[i])
        for k, to in ((0, major_to), (1, minor_to)):
            unit = up_by(u, (2 * k - 1) * MAJOR)
            unit_copy(unit, f, me, 0).wait_recv()
            unit_copy(unit, f, to, 2 + k).start()

    for i in range(1, RING):
        f = up_by(a, ORDER[i])

        @pl.when(spreads | (f < a))
        def _():
            for half in range(2):
                first_copy(f, half, me, i).wait_recv()

            @pl.when(wraps(u))
            def _():
                unit_copy(u, f, major_to, 0).start()

            @pl.when(climbs(u))
            def _():
                unit_copy(u, f, minor_to, 1).start()

    factor = math.log2(math.e) / math.sqrt(width)
    unit_step = along_y * (span * 2 * RING) + core * span * 2
    block_step = along_y * span * 2 + core * (span * 2 * RING)
    row_start = (z_at * RING + y_at) * span * 2

    def absorb(unit, order, done):
        key_block = kv[unit, :, :, 0].reshape(keys, width)
        value_block = kv[unit, :, :, 1].reshape(keys, width)
        extended = jnp.concatenate([value_block, jnp.ones_like(value_block)], axis=1)
        col = lax.broadcasted_iota(jnp.int32, (1, keys), 1)
        k_at = unit * unit_step + (col // span) * block_step + x_hi * span + col % span - row_start
        at = lax.broadcasted_iota(jnp.int32, (CH, 1), 0)

        def score(n):
            r = order[n]
            scores = factor * lax.dot_general(
                q_all[r].reshape(CH, width),
                key_block,
                (((1,), (1,)), ((), ())),
                preferred_element_type=jnp.float32,
            )
            q_at = (2 * r + at // piece) * keep + at % keep
            score_buf[n % NB] = jnp.where(k_at <= q_at, scores, NEVER)

        def weigh(n):
            take = pl.ds(pl.multiple_of(order[n] * CH, CH), CH)
            old = run_max[take, 0:1]
            top = jnp.maximum(old, jnp.max(score_buf[n % NB], axis=1, keepdims=True))
            weights = jnp.exp2(score_buf[n % NB] - top).astype(jnp.bfloat16)
            total = jnp.dot(weights, extended, preferred_element_type=jnp.float32)
            total = total + jnp.exp2(old - top) * run_acc[take, :]
            top = jnp.broadcast_to(top, (CH, width))
            if done is None:
                run_acc[take, :] = total
                run_max[take, :] = top
            else:
                done(n, total, top)

        score(0)
        for n in range(ROW):
            if n + 1 < ROW:
                score(n + 1)
            weigh(n)

    def step_of(step):
        d = (step + 1) // 2
        odd = step % 2
        unit = up_by(u, (1 - 2 * odd) * MAJOR * d)
        far = up_by(u, (2 * odd - 1) * MAJOR)
        return d, odd, unit, far

    def advance(step):
        d, odd, unit, far = step_of(step)
        to = second_peer(far)

        @pl.when(step > 0)
        def _():
            lands = (core == 1) | jnp.where(odd == 1, unit < FAR, unit < u)
            goes = (core == 1) | jnp.where(odd == 1, unit < FAR, (unit < u) & (u < RING - 1))
            goes = goes & (d < NEAR + odd * (FAR - NEAR))

            for i in range(RING):
                f = up_by(a, ORDER[i])

                @pl.when(lands & ((core == 0) | (f <= a)))
                def _():
                    unit_copy(unit, f, me, 0).wait_recv()

                    @pl.when(goes)
                    def _():
                        unit_copy(unit, f, to, step + 1).start()

        @pl.when(step == 0)
        def _():
            for i in range(1, ROW):
                slot = lax.rem(own_slot + i, ROW)
                q_copy(slot, own_slot, i).wait_recv()

        return unit, (unit <= u) | ((core == 1) & (z_at > 0))

    def turn_of(step, carry):
        unit, valid = advance(step)

        @pl.when(valid)
        def _():
            absorb(unit, range(ROW), None)

        return carry

    lax.fori_loop(0, RING - 1, turn_of, 0)
    last, valid = advance(RING - 1)

    def out_copy(slot, d, index):
        return pltpu.make_async_remote_copy(
            src_ref=out_send.at[d],
            dst_ref=out_recv.at[slot],
            send_sem=out_send_sem.at[index],
            recv_sem=out_recv_sem.at[slot],
            device_id=row_peer(d),
            device_id_type=MESH,
        )

    def stat_copy(slot, d, index):
        return pltpu.make_async_remote_copy(
            src_ref=stat_send.at[d],
            dst_ref=stat_recv.at[slot],
            send_sem=stat_send_sem.at[index],
            recv_sem=stat_recv_sem.at[slot],
            device_id=row_peer(d),
            device_id_type=MESH,
        )

    across = lax.rem(own_slot + 2, ROW)
    order = [across, across + 1 - 2 * core, own_slot + 1 - 2 * core, own_slot]

    def finish(n, total, top):
        for half in range(2):
            d = order[n] * 2 + half
            rows_of = slice(half * piece, (half + 1) * piece)
            weight = total[rows_of, width:]
            stat = top[rows_of] + math.log2(math.e) * jnp.log(weight)
            out_send[d] = (total[rows_of, :width] / weight).astype(jnp.bfloat16)
            stat_send[d] = stat.T[0:8]
            index = lax.rem(d - place + 8, 8)
            if n < ROW - 1:
                out_copy(place, d, index).start()
                stat_copy(place, d, index).start()
            else:

                @pl.when(d != place)
                def _():
                    out_copy(place, d, index).start()
                    stat_copy(place, d, index).start()

    @pl.when(valid)
    def _():
        absorb(last, order, finish)

    @pl.when(jnp.logical_not(valid))
    def _():
        for n in range(ROW):
            take = pl.ds(pl.multiple_of(order[n] * CH, CH), CH)
            finish(n, run_acc[take, :], run_max[take, :])

    keeps = [
        pltpu.make_async_copy(out_send.at[place], out_recv.at[place], store_sem.at[1]),
        pltpu.make_async_copy(stat_send.at[place], stat_recv.at[place], store_sem.at[2]),
    ]
    for copy in keeps:
        copy.start()

    out_order = (4, 5, 6, 7, 2, 3, 1)
    twin_copy(a, u, core).wait_send()
    for i in range(1, RING):

        @pl.when(spreads | (up_by(a, ORDER[i]) > a))
        def _():
            for half in range(2):
                first_copy(a, half, me, i).wait_send()

    for i in range(1, ROW):
        q_copy(own_slot, lax.rem(own_slot + i, ROW), i).wait_send()
    def drain(slot, carry):
        d = slot // 2
        odd = 1 - slot % 2
        unit = up_by(u, (1 - 2 * odd) * MAJOR * d)
        goes = (core == 1) | jnp.where(odd == 1, unit < FAR, (unit <= u) & (u < RING - 1))

        @pl.when(goes)
        def _():
            for f in range(RING):

                @pl.when((core == 0) | (f <= a))
                def _():
                    unit_copy(u, f, me, slot).wait_send()

        return carry

    lax.fori_loop(0, RING - 1, drain, 0)
    cache_store.wait()
    for i in out_order:
        slot = lax.rem(place + i, 8)
        out_copy(slot, place, i).wait_recv()
        stat_copy(slot, place, i).wait_recv()

    for i in out_order:
        out_copy(place, lax.rem(place + i, 8), i).wait_send()
        stat_copy(place, lax.rem(place + i, 8), i).wait_send()
    for copy in keeps:
        copy.wait()


def merge_kernel(heads, group, out_recv, stat_recv, cache_in, att, cache, wide_out):
    _, piece, width = out_recv.shape
    keep = piece // group
    cache[...] = cache_in[...]
    for core_from in range(2):
        for tp_from in range(2):
            low = core_from * 2 + tp_from
            wide_stat = [
                jnp.broadcast_to(stat_recv[s, 0:1, :], (piece, width)).T for s in (low, low + 4)
            ]
            gap = wide_stat[1] - wide_stat[0]
            merged = out_recv[low].astype(jnp.float32) / (1.0 + jnp.exp2(gap))
            merged = merged + out_recv[low + 4].astype(jnp.float32) / (1.0 + jnp.exp2(-gap))
            for g in range(group):
                head = tp_from * heads + core_from * group + g
                wide_out[pl.ds(head, keep, stride=2 * heads), :] = merged[g * keep : (g + 1) * keep]
    att[...] = wide_out[...].astype(jnp.bfloat16)


def build(ctx_size, queries, keys_in, values_in):
    rows, heads, width = queries.shape
    kv_heads = keys_in.shape[1]
    group = heads // kv_heads
    keep = rows // 2
    piece = group * keep
    fine, coarse = angle_tables(ctx_size, rows, width)
    f32, bf16 = jnp.float32, jnp.bfloat16

    hbm = pl.BlockSpec(memory_space=pl.ANY)
    dma = pltpu.SemaphoreType.DMA
    parts, stats, cache = pl.pallas_call(
        functools.partial(kernel, heads, kv_heads),
        out_shape=(
            jax.ShapeDtypeStruct((8, piece, width), bf16),
            jax.ShapeDtypeStruct((8, 8, piece), f32),
            jax.ShapeDtypeStruct((rows * kv_heads, width), bf16),
        ),
        in_specs=[hbm] * 5,
        out_specs=(hbm, hbm, hbm),
        scratch_shapes=[
            pltpu.VMEM((rows * heads, width), bf16),
            pltpu.VMEM((rows * kv_heads, width), bf16),
            pltpu.VMEM((rows * kv_heads, width), bf16),
            pltpu.VMEM((2, rows, width), f32),
            pltpu.VMEM((2, 8, width), f32),
            pltpu.VMEM((2, rows * kv_heads, width), f32),
            pltpu.VMEM((rows * heads, width), f32),
            pltpu.VMEM((kv_heads, 2, rows, width), bf16),
            pltpu.VMEM((RING, RING, 2, 2, rows, width), bf16),
            pltpu.VMEM((2, 2, group, keep, width), bf16),
            pltpu.VMEM((ROW, 2, group, keep, width), bf16),
            pltpu.VMEM((8 * piece, width), f32),
            pltpu.VMEM((8 * piece, 2 * width), f32),
            pltpu.VMEM((NB, CH, RING * 2 * rows), f32),
            pltpu.VMEM((8, piece, width), bf16),
            pltpu.VMEM((8, 8, piece), f32),
            pltpu.VMEM((rows * kv_heads, width), bf16),
            dma((5,)),
            dma((3,)),
            dma,
            dma,
            dma((2 * RING, 2)),
            dma((RING, 2)),
            dma((RING, RING)),
            dma((RING, RING)),
            dma((ROW,)),
            dma((ROW,)),
            dma((8,)),
            dma((8,)),
            dma((8,)),
            dma((8,)),
        ],
        compiler_params=pltpu.CompilerParams(collective_id=0, has_side_effects=True),
    )(
        queries.reshape(rows * heads, width),
        keys_in.reshape(rows * kv_heads, width),
        values_in.reshape(rows * kv_heads, width),
        jnp.asarray(fine),
        jnp.asarray(coarse),
    )
    vmem = pl.BlockSpec(memory_space=pltpu.VMEM)
    att, cache = pl.pallas_call(
        functools.partial(merge_kernel, heads, group),
        out_shape=(
            jax.ShapeDtypeStruct((2 * heads * keep, width), bf16),
            jax.ShapeDtypeStruct((rows * kv_heads, width), bf16),
        ),
        in_specs=[vmem] * 3,
        out_specs=(vmem, vmem),
        scratch_shapes=[pltpu.VMEM((2 * heads * keep, width), f32)],
    )(parts, stats, cache)
    return att.reshape(keep, 2 * heads, width), cache.reshape(rows, kv_heads, width)


def solution(mesh):
    ctx_size = mesh.shape["ctx"]

    def per_device(queries, incoming_lookup_vectors, incoming_content_vectors):
        return build(ctx_size, queries, incoming_lookup_vectors, incoming_content_vectors)

    return jax.shard_map(
        per_device,
        mesh=mesh,
        in_specs=(P("ctx", "tp", None), P("ctx", "tp", None), P("ctx", "tp", None)),
        out_specs=(P(("ctx", "tp"), None, None), P("ctx", "tp", None)),
        check_vma=False,
    )
```

```python
import functools
import math

import jax
import jax.numpy as jnp
import numpy as np
from jax import lax
from jax.experimental import pallas as pl
from jax.experimental.pallas import tpu as pltpu
from jax.sharding import PartitionSpec as P

rope_base = 500000.0
MESH = pl.DeviceIdType.MESH
ROW = 4
RING = 8
ORDER = (0, 1, 7, 2, 6, 3, 5, 4)
MAJOR = -1
FAR, NEAR = 4, 3
NEVER = -1e30
CH, NB = 256, 2


def angle_tables(blocks, rows, width):
    half = width // 2
    freq = rope_base ** (-(np.arange(half, dtype=np.float64) * 2.0 / width))
    freq = np.concatenate([freq, freq])[None, :]
    fine = np.arange(rows, dtype=np.float64)[:, None] * freq
    coarse = np.arange(blocks, dtype=np.float64)[:, None] * rows * freq
    fine_table = np.stack([np.cos(fine), np.sin(fine)]).astype(np.float32)
    coarse_table = np.stack([np.cos(coarse), np.sin(coarse)], 1).astype(np.float32)
    coarse_table = np.broadcast_to(coarse_table[:, :, None, :], (blocks, 2, 8, width))
    return fine_table, np.ascontiguousarray(coarse_table)


def kernel(
    heads,
    kv_heads,
    q_hbm,
    k_hbm,
    v_hbm,
    fine_hbm,
    coarse_hbm,
    out_recv,
    stat_recv,
    cache_hbm,
    q_in,
    k_in,
    v_in,
    fine,
    coarse,
    wide_kv,
    wide_q,
    kv_own,
    kv,
    q_send,
    q_all,
    run_max,
    run_acc,
    score_buf,
    out_send,
    stat_send,
    cache_vmem,
    load_sem,
    store_sem,
    twin_send,
    twin_recv,
    first_send,
    first_recv,
    unit_send,
    unit_recv,
    q_send_sem,
    q_recv_sem,
    out_send_sem,
    out_recv_sem,
    stat_send_sem,
    stat_recv_sem,
):
    rows = k_in.shape[0] // kv_heads
    width = k_in.shape[1]
    half_width = width // 2
    group = heads // kv_heads
    keep = rows // 2
    span = 2 * rows
    piece = group * keep
    keys = RING * span
    me = lax.axis_index("ctx")
    part = lax.axis_index("tp")
    core = me % 2
    x_hi = (me // 2) % 2
    y_at = (me // ROW) % RING
    z_at = me // (ROW * RING)
    along_y = 1 - core
    a = along_y * y_at + core * z_at
    u = along_y * z_at + core * y_at
    first_stride = along_y * ROW + core * ROW * RING
    second_stride = along_y * ROW * RING + core * ROW
    row_base = me - me % ROW
    twin = me + 1 - 2 * core
    place = (me % ROW) * 2 + part

    def first_peer(f):
        return me + (f - a) * first_stride

    def second_peer(w):
        return me + (w - u) * second_stride

    def up_by(value, d):
        return lax.rem(value + d + RING, RING)

    def row_peer(d):
        return {"ctx": row_base + d // 2, "tp": d % 2}

    loads = [
        pltpu.make_async_copy(k_hbm, k_in, load_sem.at[0]),
        pltpu.make_async_copy(v_hbm, v_in, load_sem.at[1]),
        pltpu.make_async_copy(fine_hbm, fine, load_sem.at[2]),
        pltpu.make_async_copy(coarse_hbm.at[me], coarse, load_sem.at[3]),
        pltpu.make_async_copy(q_hbm, q_in, load_sem.at[4]),
    ]
    barrier = pltpu.get_barrier_semaphore()
    for d in range(1, RING):
        to = first_peer(up_by(a, d))
        pl.semaphore_signal(barrier, inc=1, device_id={"ctx": to}, device_id_type=MESH)
    for d in (1, -1):
        to = second_peer(up_by(u, d))
        pl.semaphore_signal(barrier, inc=1, device_id={"ctx": to}, device_id_type=MESH)
    for i in range(1, 8):
        to = row_peer(lax.rem(place + i, 8))
        pl.semaphore_signal(barrier, inc=1, device_id=to, device_id_type=MESH)

    for load in loads:
        load.start()

    loads[2].wait()
    loads[3].wait()
    cos_c = coarse[0, 0:1, :]
    sin_c = coarse[1, 0:1, :]
    cosine = cos_c * fine[0] - sin_c * fine[1]
    sine = sin_c * fine[0] + cos_c * fine[1]
    lane = lax.broadcasted_iota(jnp.int32, (rows, width), 1)
    sine = jnp.where(lane < half_width, -sine, sine)

    def turn(x):
        return x * cosine + pltpu.roll(x, half_width, 1) * sine

    loads[0].wait()
    loads[1].wait()
    wide_kv[0] = k_in[...].astype(jnp.float32)
    wide_kv[1] = v_in[...].astype(jnp.float32)
    for j in range(kv_heads):
        take = pl.ds(j, rows, stride=kv_heads)
        key_rot = turn(wide_kv[0, take, :])
        wide_kv[0, take, :] = key_rot
        kv_own[j, 0] = key_rot.astype(jnp.bfloat16)
        kv_own[j, 1] = wide_kv[1, take, :].astype(jnp.bfloat16)
    kv[u, a, core] = kv_own[core]
    cache_vmem[...] = wide_kv[0].astype(jnp.bfloat16)
    cache_store = pltpu.make_async_copy(cache_vmem, cache_hbm, store_sem.at[0])
    cache_store.start()
    pl.semaphore_wait(barrier, (RING - 1) + 2 + 7)

    def twin_copy(unit, f, half):
        return pltpu.make_async_remote_copy(
            src_ref=kv_own.at[1 - core],
            dst_ref=kv.at[unit, f, half],
            send_sem=twin_send,
            recv_sem=twin_recv,
            device_id={"ctx": twin},
            device_id_type=MESH,
        )

    def first_copy(f, half, to, slot):
        return pltpu.make_async_remote_copy(
            src_ref=kv.at[u, f, half],
            dst_ref=kv.at[u, f, half],
            send_sem=first_send.at[slot, half],
            recv_sem=first_recv.at[f, half],
            device_id={"ctx": to},
            device_id_type=MESH,
        )

    def unit_copy(unit, f, to, slot):
        return pltpu.make_async_remote_copy(
            src_ref=kv.at[unit, f],
            dst_ref=kv.at[unit, f],
            send_sem=unit_send.at[slot, f],
            recv_sem=unit_recv.at[unit, f],
            device_id={"ctx": to},
            device_id_type=MESH,
        )

    def q_copy(slot, to_slot, index):
        return pltpu.make_async_remote_copy(
            src_ref=q_send.at[to_slot % 2],
            dst_ref=q_all.at[slot],
            send_sem=q_send_sem.at[index],
            recv_sem=q_recv_sem.at[slot],
            device_id={"ctx": row_base + to_slot},
            device_id_type=MESH,
        )

    def shares(unit):
        return ((core == 0) & (unit == 3)) | ((core == 1) & (a == RING - 1))

    spreads = (core == 0) & (u < RING - 1)

    def climbs(unit):
        return (core == 1) | ((unit <= u) & (u < RING - 1))

    def wraps(unit):
        return (core == 1) | (unit < FAR)

    def spread(half, i_list):
        for i in i_list:
            to = up_by(a, ORDER[i])

            @pl.when(spreads | (to > a))
            def _():
                first_copy(a, half, first_peer(to), i).start()


    major_to = second_peer(up_by(u, MAJOR))
    minor_to = second_peer(up_by(u, -MAJOR))

    twin_copy(a, u, core).start()
    spread(core, (1, 2, 3, 4, 5, 6, 7))

    own_slot = me % ROW
    loads[4].wait()
    wide_q[...] = q_in[...].astype(jnp.float32)
    for h in range(heads):
        turned = turn(wide_q[pl.ds(h, rows, stride=heads), :]).astype(jnp.bfloat16)
        for half in range(2):
            q_send[h // group, half, h % group] = turned[half * keep : (half + 1) * keep]

    twin_copy(u, a, 1 - core).wait_recv()
    spread(1 - core, (1, 2, 3, 4, 5, 6, 7))
    pl.when(wraps(u))(lambda: unit_copy(u, a, major_to, 0).start())
    pl.when(climbs(u))(lambda: unit_copy(u, a, minor_to, 1).start())
    for i in range(1, ROW):
        q_copy(own_slot, lax.rem(own_slot + i, ROW), i).start()
    q_all[own_slot] = q_send[core]
    @pl.when((core == 0) & (u == RING - 1))
    def _():
        def clear(f, carry):
            kv[u, f] = jnp.zeros((2, 2, rows, width), jnp.bfloat16)
            return carry

        lax.fori_loop(a + 1, RING, clear, 0)

    @pl.when(core == 1)
    def _():
        def clear(f, carry):
            kv[:, f] = jnp.zeros((RING, 2, 2, rows, width), jnp.bfloat16)
            return carry

        lax.fori_loop(a + 1, RING, clear, 0)

    run_max[...] = jnp.full(run_max.shape, NEVER, jnp.float32)
    run_acc[...] = jnp.zeros(run_acc.shape, jnp.float32)

    def next_hop(i):
        return first_peer(up_by(a, 1 if ORDER[i] > RING // 2 else -1))

    def pass_on(f, half, i, slot):
        first_copy(f, half, next_hop(i), slot).start()
        first_sends.append((half, slot))

    def early(i):
        f = up_by(a, ORDER[i])
        for k, to in ((0, major_to), (1, minor_to)):
            unit = up_by(u, (2 * k - 1) * MAJOR)
            unit_copy(unit, f, me, 0).wait_recv()
            unit_copy(unit, f, to, 2 + k).start()

    for i in range(1, RING):
        f = up_by(a, ORDER[i])

        @pl.when(spreads | (f < a))
        def _():
            for half in range(2):
                first_copy(f, half, me, i).wait_recv()

            @pl.when(wraps(u))
            def _():
                unit_copy(u, f, major_to, 0).start()

            @pl.when(climbs(u))
            def _():
                unit_copy(u, f, minor_to, 1).start()

    factor = math.log2(math.e) / math.sqrt(width)
    unit_step = along_y * (span * 2 * RING) + core * span * 2
    block_step = along_y * span * 2 + core * (span * 2 * RING)
    row_start = (z_at * RING + y_at) * span * 2

    def absorb(unit, order, done):
        key_block = kv[unit, :, :, 0].reshape(keys, width)
        value_block = kv[unit, :, :, 1].reshape(keys, width)
        extended = jnp.concatenate([value_block, jnp.ones_like(value_block)], axis=1)
        col = lax.broadcasted_iota(jnp.int32, (1, keys), 1)
        k_at = unit * unit_step + (col // span) * block_step + x_hi * span + col % span - row_start
        at = lax.broadcasted_iota(jnp.int32, (CH, 1), 0)

        def score(n):
            r = order[n]
            scores = factor * lax.dot_general(
                q_all[r].reshape(CH, width),
                key_block,
                (((1,), (1,)), ((), ())),
                preferred_element_type=jnp.float32,
            )
            q_at = (2 * r + at // piece) * keep + at % keep
            score_buf[n % NB] = jnp.where(k_at <= q_at, scores, NEVER)

        def weigh(n):
            take = pl.ds(pl.multiple_of(order[n] * CH, CH), CH)
            old = run_max[take, 0:1]
            top = jnp.maximum(old, jnp.max(score_buf[n % NB], axis=1, keepdims=True))
            weights = jnp.exp2(score_buf[n % NB] - top).astype(jnp.bfloat16)
            total = jnp.dot(weights, extended, preferred_element_type=jnp.float32)
            total = total + jnp.exp2(old - top) * run_acc[take, :]
            top = jnp.broadcast_to(top, (CH, width))
            if done is None:
                run_acc[take, :] = total
                run_max[take, :] = top
            else:
                done(n, total, top)

        score(0)
        for n in range(len(order)):
            if n + 1 < len(order):
                score(n + 1)
            weigh(n)

    def unit_at(d, odd):
        return up_by(u, (1 - 2 * odd) * MAJOR * d)

    def counts(unit):
        return (unit <= u) | ((core == 1) & (z_at > 0))

    def event(d, odd, i):
        unit = unit_at(d, odd)
        f = up_by(a, ORDER[i])
        early = 1 if i < RING // 2 else 0
        if odd:
            lands = goes = (core == 1) | (unit < FAR)
            to = major_to
        else:
            lands = (core == 1) | (unit < u)
            goes = (core == 1) | ((unit < u) & (u < RING - 1))
            to = minor_to
        onward = goes & ((d < NEAR) | ((d == NEAR) & (odd == jnp.where(shares(unit), early, 1))))

        @pl.when(lands & ((core == 0) | (f <= a)))
        def _():
            unit_copy(unit, f, me, 0).wait_recv()

            @pl.when(onward)
            def _():
                unit_copy(unit, f, to, 2 * d + 1 - odd).start()

    def weave(d, d_ready, sides):
        for g in range(4):
            for i in range(g * 2, (g + 1) * 2):
                for odd in sides:
                    event(d, odd, i)
            odd = 1 - g // 2
            unit = unit_at(d_ready, odd)
            part_of = range(g % 2 * 2, (g % 2 + 1) * 2)

            @pl.when(counts(unit) & ((d_ready > 0) | (odd == 1)))
            def _():
                absorb(unit, part_of, None)

    for i in range(1, ROW):
        slot = lax.rem(own_slot + i, ROW)
        q_copy(slot, own_slot, i).wait_recv()

    def stage(d, carry):
        weave(d, d - 1, (1, 0))
        return carry

    lax.fori_loop(1, NEAR + 1, stage, 0)
    weave(FAR, NEAR, (1,))
    last = unit_at(FAR, 1)
    valid = counts(last)

    def out_copy(slot, d, index):
        return pltpu.make_async_remote_copy(
            src_ref=out_send.at[d],
            dst_ref=out_recv.at[slot],
            send_sem=out_send_sem.at[index],
            recv_sem=out_recv_sem.at[slot],
            device_id=row_peer(d),
            device_id_type=MESH,
        )

    def stat_copy(slot, d, index):
        return pltpu.make_async_remote_copy(
            src_ref=stat_send.at[d],
            dst_ref=stat_recv.at[slot],
            send_sem=stat_send_sem.at[index],
            recv_sem=stat_recv_sem.at[slot],
            device_id=row_peer(d),
            device_id_type=MESH,
        )

    across = lax.rem(own_slot + 2, ROW)
    order = [across, across + 1 - 2 * core, own_slot + 1 - 2 * core, own_slot]

    def finish(n, total, top):
        for half in range(2):
            d = order[n] * 2 + half
            rows_of = slice(half * piece, (half + 1) * piece)
            weight = total[rows_of, width:]
            stat = top[rows_of] + math.log2(math.e) * jnp.log(weight)
            out_send[d] = (total[rows_of, :width] / weight).astype(jnp.bfloat16)
            stat_send[d] = stat.T[0:8]
            index = lax.rem(d - place + 8, 8)
            if n < ROW - 1:
                out_copy(place, d, index).start()
                stat_copy(place, d, index).start()
            else:

                @pl.when(d != place)
                def _():
                    out_copy(place, d, index).start()
                    stat_copy(place, d, index).start()

    @pl.when(valid)
    def _():
        absorb(last, order, finish)

    @pl.when(jnp.logical_not(valid))
    def _():
        for n in range(ROW):
            take = pl.ds(pl.multiple_of(order[n] * CH, CH), CH)
            finish(n, run_acc[take, :], run_max[take, :])

    keeps = [
        pltpu.make_async_copy(out_send.at[place], out_recv.at[place], store_sem.at[1]),
        pltpu.make_async_copy(stat_send.at[place], stat_recv.at[place], store_sem.at[2]),
    ]
    for copy in keeps:
        copy.start()

    out_order = (4, 5, 6, 7, 2, 3, 1)
    twin_copy(a, u, core).wait_send()
    for i in range(1, RING):

        @pl.when(spreads | (up_by(a, ORDER[i]) > a))
        def _():
            for half in range(2):
                first_copy(a, half, me, i).wait_send()

    for i in range(1, ROW):
        q_copy(own_slot, lax.rem(own_slot + i, ROW), i).wait_send()
    def drain(slot, carry):
        d = slot // 2
        odd = 1 - slot % 2
        unit = up_by(u, (1 - 2 * odd) * MAJOR * d)
        goes = (core == 1) | jnp.where(odd == 1, unit < FAR, (unit <= u) & (u < RING - 1))

        @pl.when(goes)
        def _():
            for i in range(RING):
                f = up_by(a, ORDER[i])
                early = 1 if i < RING // 2 else 0
                sent = (d < NEAR) | (odd == jnp.where(shares(unit), early, 1))

                @pl.when(sent & ((core == 0) | (f <= a)))
                def _():
                    unit_copy(u, f, me, slot).wait_send()

        return carry

    lax.fori_loop(0, RING, drain, 0)
    cache_store.wait()
    for i in out_order:
        slot = lax.rem(place + i, 8)
        out_copy(slot, place, i).wait_recv()
        stat_copy(slot, place, i).wait_recv()

    for i in out_order:
        out_copy(place, lax.rem(place + i, 8), i).wait_send()
        stat_copy(place, lax.rem(place + i, 8), i).wait_send()
    for copy in keeps:
        copy.wait()


def merge_kernel(heads, group, out_recv, stat_recv, cache_in, att, cache, wide_out):
    _, piece, width = out_recv.shape
    keep = piece // group
    cache[...] = cache_in[...]
    for core_from in range(2):
        for tp_from in range(2):
            low = core_from * 2 + tp_from
            wide_stat = [
                jnp.broadcast_to(stat_recv[s, 0:1, :], (piece, width)).T for s in (low, low + 4)
            ]
            gap = wide_stat[1] - wide_stat[0]
            merged = out_recv[low].astype(jnp.float32) / (1.0 + jnp.exp2(gap))
            merged = merged + out_recv[low + 4].astype(jnp.float32) / (1.0 + jnp.exp2(-gap))
            for g in range(group):
                head = tp_from * heads + core_from * group + g
                wide_out[pl.ds(head, keep, stride=2 * heads), :] = merged[g * keep : (g + 1) * keep]
    att[...] = wide_out[...].astype(jnp.bfloat16)


def build(ctx_size, queries, keys_in, values_in):
    rows, heads, width = queries.shape
    kv_heads = keys_in.shape[1]
    group = heads // kv_heads
    keep = rows // 2
    piece = group * keep
    fine, coarse = angle_tables(ctx_size, rows, width)
    f32, bf16 = jnp.float32, jnp.bfloat16

    hbm = pl.BlockSpec(memory_space=pl.ANY)
    dma = pltpu.SemaphoreType.DMA
    parts, stats, cache = pl.pallas_call(
        functools.partial(kernel, heads, kv_heads),
        out_shape=(
            jax.ShapeDtypeStruct((8, piece, width), bf16),
            jax.ShapeDtypeStruct((8, 8, piece), f32),
            jax.ShapeDtypeStruct((rows * kv_heads, width), bf16),
        ),
        in_specs=[hbm] * 5,
        out_specs=(hbm, hbm, hbm),
        scratch_shapes=[
            pltpu.VMEM((rows * heads, width), bf16),
            pltpu.VMEM((rows * kv_heads, width), bf16),
            pltpu.VMEM((rows * kv_heads, width), bf16),
            pltpu.VMEM((2, rows, width), f32),
            pltpu.VMEM((2, 8, width), f32),
            pltpu.VMEM((2, rows * kv_heads, width), f32),
            pltpu.VMEM((rows * heads, width), f32),
            pltpu.VMEM((kv_heads, 2, rows, width), bf16),
            pltpu.VMEM((RING, RING, 2, 2, rows, width), bf16),
            pltpu.VMEM((2, 2, group, keep, width), bf16),
            pltpu.VMEM((ROW, 2, group, keep, width), bf16),
            pltpu.VMEM((8 * piece, width), f32),
            pltpu.VMEM((8 * piece, 2 * width), f32),
            pltpu.VMEM((NB, CH, RING * 2 * rows), f32),
            pltpu.VMEM((8, piece, width), bf16),
            pltpu.VMEM((8, 8, piece), f32),
            pltpu.VMEM((rows * kv_heads, width), bf16),
            dma((5,)),
            dma((3,)),
            dma,
            dma,
            dma((2 * RING, 2)),
            dma((RING, 2)),
            dma((RING, RING)),
            dma((RING, RING)),
            dma((ROW,)),
            dma((ROW,)),
            dma((8,)),
            dma((8,)),
            dma((8,)),
            dma((8,)),
        ],
        compiler_params=pltpu.CompilerParams(collective_id=0, has_side_effects=True),
    )(
        queries.reshape(rows * heads, width),
        keys_in.reshape(rows * kv_heads, width),
        values_in.reshape(rows * kv_heads, width),
        jnp.asarray(fine),
        jnp.asarray(coarse),
    )
    vmem = pl.BlockSpec(memory_space=pltpu.VMEM)
    att, cache = pl.pallas_call(
        functools.partial(merge_kernel, heads, group),
        out_shape=(
            jax.ShapeDtypeStruct((2 * heads * keep, width), bf16),
            jax.ShapeDtypeStruct((rows * kv_heads, width), bf16),
        ),
        in_specs=[vmem] * 3,
        out_specs=(vmem, vmem),
        scratch_shapes=[pltpu.VMEM((2 * heads * keep, width), f32)],
    )(parts, stats, cache)
    return att.reshape(keep, 2 * heads, width), cache.reshape(rows, kv_heads, width)


def solution(mesh):
    ctx_size = mesh.shape["ctx"]

    def per_device(queries, incoming_lookup_vectors, incoming_content_vectors):
        return build(ctx_size, queries, incoming_lookup_vectors, incoming_content_vectors)

    return jax.shard_map(
        per_device,
        mesh=mesh,
        in_specs=(P("ctx", "tp", None), P("ctx", "tp", None), P("ctx", "tp", None)),
        out_specs=(P(("ctx", "tp"), None, None), P("ctx", "tp", None)),
        check_vma=False,
    )
```

```python
import functools
import math

import jax
import jax.numpy as jnp
import numpy as np
from jax import lax
from jax.experimental import pallas as pl
from jax.experimental.pallas import tpu as pltpu
from jax.sharding import PartitionSpec as P

rope_base = 500000.0
MESH = pl.DeviceIdType.MESH
ROW = 4
RING = 8
ORDER = (0, 1, 7, 2, 6, 3, 5, 4)
MAJOR = -1
FAR, NEAR = 4, 3
NEVER = -1e30
CH, NB = 256, 2


def angle_tables(blocks, rows, width):
    half = width // 2
    freq = rope_base ** (-(np.arange(half, dtype=np.float64) * 2.0 / width))
    freq = np.concatenate([freq, freq])[None, :]
    fine = np.arange(rows, dtype=np.float64)[:, None] * freq
    coarse = np.arange(blocks, dtype=np.float64)[:, None] * rows * freq
    fine_table = np.stack([np.cos(fine), np.sin(fine)]).astype(np.float32)
    coarse_table = np.stack([np.cos(coarse), np.sin(coarse)], 1).astype(np.float32)
    coarse_table = np.broadcast_to(coarse_table[:, :, None, :], (blocks, 2, 8, width))
    return fine_table, np.ascontiguousarray(coarse_table)


def kernel(
    heads,
    kv_heads,
    q_hbm,
    k_hbm,
    v_hbm,
    fine_hbm,
    coarse_hbm,
    out_recv,
    stat_recv,
    cache_hbm,
    q_in,
    k_in,
    v_in,
    fine,
    coarse,
    wide_kv,
    wide_q,
    kv_own,
    kv,
    q_send,
    q_all,
    run_max,
    run_acc,
    score_buf,
    out_send,
    stat_send,
    cache_vmem,
    load_sem,
    store_sem,
    twin_send,
    twin_recv,
    first_send,
    first_recv,
    unit_send,
    unit_recv,
    q_send_sem,
    q_recv_sem,
    out_send_sem,
    out_recv_sem,
    stat_send_sem,
    stat_recv_sem,
):
    rows = k_in.shape[0] // kv_heads
    width = k_in.shape[1]
    half_width = width // 2
    group = heads // kv_heads
    keep = rows // 2
    span = 2 * rows
    piece = group * keep
    keys = RING * span
    me = lax.axis_index("ctx")
    part = lax.axis_index("tp")
    core = me % 2
    x_hi = (me // 2) % 2
    y_at = (me // ROW) % RING
    z_at = me // (ROW * RING)
    along_y = 1 - core
    a = along_y * y_at + core * z_at
    u = along_y * z_at + core * y_at
    first_stride = along_y * ROW + core * ROW * RING
    second_stride = along_y * ROW * RING + core * ROW
    row_base = me - me % ROW
    twin = me + 1 - 2 * core
    place = (me % ROW) * 2 + part

    def first_peer(f):
        return me + (f - a) * first_stride

    def second_peer(w):
        return me + (w - u) * second_stride

    def up_by(value, d):
        return lax.rem(value + d + RING, RING)

    def row_peer(d):
        return {"ctx": row_base + d // 2, "tp": d % 2}

    loads = [
        pltpu.make_async_copy(k_hbm, k_in, load_sem.at[0]),
        pltpu.make_async_copy(v_hbm, v_in, load_sem.at[1]),
        pltpu.make_async_copy(fine_hbm, fine, load_sem.at[2]),
        pltpu.make_async_copy(coarse_hbm.at[me], coarse, load_sem.at[3]),
        pltpu.make_async_copy(q_hbm, q_in, load_sem.at[4]),
    ]
    for load in loads:
        load.start()

    barrier = pltpu.get_barrier_semaphore()
    for d in range(1, RING):
        to = first_peer(up_by(a, d))
        pl.semaphore_signal(barrier, inc=1, device_id={"ctx": to}, device_id_type=MESH)
    for d in (1, -1):
        to = second_peer(up_by(u, d))
        pl.semaphore_signal(barrier, inc=1, device_id={"ctx": to}, device_id_type=MESH)
    for i in range(1, 8):
        to = row_peer(lax.rem(place + i, 8))
        pl.semaphore_signal(barrier, inc=1, device_id=to, device_id_type=MESH)


    loads[2].wait()
    loads[3].wait()
    cos_c = coarse[0, 0:1, :]
    sin_c = coarse[1, 0:1, :]
    cosine = cos_c * fine[0] - sin_c * fine[1]
    sine = sin_c * fine[0] + cos_c * fine[1]
    lane = lax.broadcasted_iota(jnp.int32, (rows, width), 1)
    sine = jnp.where(lane < half_width, -sine, sine)

    def turn(x):
        return x * cosine + pltpu.roll(x, half_width, 1) * sine

    loads[0].wait()
    loads[1].wait()
    wide_kv[0] = k_in[...].astype(jnp.float32)
    wide_kv[1] = v_in[...].astype(jnp.float32)
    for j in range(kv_heads):
        take = pl.ds(j, rows, stride=kv_heads)
        key_rot = turn(wide_kv[0, take, :])
        wide_kv[0, take, :] = key_rot
        kv_own[j, 0] = key_rot.astype(jnp.bfloat16)
        kv_own[j, 1] = wide_kv[1, take, :].astype(jnp.bfloat16)
    kv[u, a, core] = kv_own[core]
    pl.semaphore_wait(barrier, (RING - 1) + 2 + 7)

    def twin_copy(unit, f, half):
        return pltpu.make_async_remote_copy(
            src_ref=kv_own.at[1 - core],
            dst_ref=kv.at[unit, f, half],
            send_sem=twin_send,
            recv_sem=twin_recv,
            device_id={"ctx": twin},
            device_id_type=MESH,
        )

    def first_copy(f, half, to, slot):
        return pltpu.make_async_remote_copy(
            src_ref=kv.at[u, f, half],
            dst_ref=kv.at[u, f, half],
            send_sem=first_send.at[slot, half],
            recv_sem=first_recv.at[f, half],
            device_id={"ctx": to},
            device_id_type=MESH,
        )

    def unit_copy(unit, f, to, slot):
        return pltpu.make_async_remote_copy(
            src_ref=kv.at[unit, f],
            dst_ref=kv.at[unit, f],
            send_sem=unit_send.at[slot, f],
            recv_sem=unit_recv.at[unit, f],
            device_id={"ctx": to},
            device_id_type=MESH,
        )

    def q_copy(slot, to_slot, index):
        return pltpu.make_async_remote_copy(
            src_ref=q_send.at[to_slot % 2],
            dst_ref=q_all.at[slot],
            send_sem=q_send_sem.at[index],
            recv_sem=q_recv_sem.at[slot],
            device_id={"ctx": row_base + to_slot},
            device_id_type=MESH,
        )

    def shares(unit):
        return ((core == 0) & (unit == 3)) | ((core == 1) & (a == RING - 1))

    spreads = (core == 0) & (u < RING - 1)

    def climbs(unit):
        return (core == 1) | ((unit <= u) & (u < RING - 1))

    def wraps(unit):
        return (core == 1) | (unit < FAR)

    def spread(half, i_list):
        for i in i_list:
            to = up_by(a, ORDER[i])

            @pl.when(spreads | (to > a))
            def _():
                first_copy(a, half, first_peer(to), i).start()


    major_to = second_peer(up_by(u, MAJOR))
    minor_to = second_peer(up_by(u, -MAJOR))

    twin_copy(a, u, core).start()
    spread(core, (1, 2, 3, 4, 5, 6, 7))

    cache_vmem[...] = wide_kv[0].astype(jnp.bfloat16)
    cache_store = pltpu.make_async_copy(cache_vmem, cache_hbm, store_sem.at[0])
    cache_store.start()
    own_slot = me % ROW
    loads[4].wait()
    wide_q[...] = q_in[...].astype(jnp.float32)
    for h in range(heads):
        turned = turn(wide_q[pl.ds(h, rows, stride=heads), :]).astype(jnp.bfloat16)
        for half in range(2):
            q_send[h // group, half, h % group] = turned[half * keep : (half + 1) * keep]

    twin_copy(u, a, 1 - core).wait_recv()
    spread(1 - core, (1, 2, 3, 4, 5, 6, 7))
    pl.when(wraps(u))(lambda: unit_copy(u, a, major_to, 0).start())
    pl.when(climbs(u))(lambda: unit_copy(u, a, minor_to, 1).start())
    for i in range(1, ROW):
        q_copy(own_slot, lax.rem(own_slot + i, ROW), i).start()
    q_all[own_slot] = q_send[core]
    @pl.when((core == 0) & (u == RING - 1))
    def _():
        def clear(f, carry):
            kv[u, f] = jnp.zeros((2, 2, rows, width), jnp.bfloat16)
            return carry

        lax.fori_loop(a + 1, RING, clear, 0)

    @pl.when(core == 1)
    def _():
        def clear(f, carry):
            kv[:, f] = jnp.zeros((RING, 2, 2, rows, width), jnp.bfloat16)
            return carry

        lax.fori_loop(a + 1, RING, clear, 0)

    run_max[...] = jnp.full(run_max.shape, NEVER, jnp.float32)
    run_acc[...] = jnp.zeros(run_acc.shape, jnp.float32)

    def next_hop(i):
        return first_peer(up_by(a, 1 if ORDER[i] > RING // 2 else -1))

    def pass_on(f, half, i, slot):
        first_copy(f, half, next_hop(i), slot).start()
        first_sends.append((half, slot))

    def early(i):
        f = up_by(a, ORDER[i])
        for k, to in ((0, major_to), (1, minor_to)):
            unit = up_by(u, (2 * k - 1) * MAJOR)
            unit_copy(unit, f, me, 0).wait_recv()
            unit_copy(unit, f, to, 2 + k).start()

    for i in range(1, RING):
        f = up_by(a, ORDER[i])

        @pl.when(spreads | (f < a))
        def _():
            for half in range(2):
                first_copy(f, half, me, i).wait_recv()

            @pl.when(wraps(u))
            def _():
                unit_copy(u, f, major_to, 0).start()

            @pl.when(climbs(u))
            def _():
                unit_copy(u, f, minor_to, 1).start()

    factor = math.log2(math.e) / math.sqrt(width)
    unit_step = along_y * (span * 2 * RING) + core * span * 2
    block_step = along_y * span * 2 + core * (span * 2 * RING)
    row_start = (z_at * RING + y_at) * span * 2

    def absorb(unit, order, done):
        key_block = kv[unit, :, :, 0].reshape(keys, width)
        value_block = kv[unit, :, :, 1].reshape(keys, width)
        extended = jnp.concatenate([value_block, jnp.ones_like(value_block)], axis=1)
        col = lax.broadcasted_iota(jnp.int32, (1, keys), 1)
        k_at = unit * unit_step + (col // span) * block_step + x_hi * span + col % span - row_start
        at = lax.broadcasted_iota(jnp.int32, (CH, 1), 0)

        def score(n):
            r = order[n]
            scores = factor * lax.dot_general(
                q_all[r].reshape(CH, width),
                key_block,
                (((1,), (1,)), ((), ())),
                preferred_element_type=jnp.float32,
            )
            q_at = (2 * r + at // piece) * keep + at % keep
            score_buf[n % NB] = jnp.where(k_at <= q_at, scores, NEVER)

        def weigh(n):
            take = pl.ds(pl.multiple_of(order[n] * CH, CH), CH)
            old = run_max[take, 0:1]
            top = jnp.maximum(old, jnp.max(score_buf[n % NB], axis=1, keepdims=True))
            weights = jnp.exp2(score_buf[n % NB] - top).astype(jnp.bfloat16)
            total = jnp.dot(weights, extended, preferred_element_type=jnp.float32)
            total = total + jnp.exp2(old - top) * run_acc[take, :]
            top = jnp.broadcast_to(top, (CH, width))
            if done is None:
                run_acc[take, :] = total
                run_max[take, :] = top
            else:
                done(n, total, top)

        score(0)
        for n in range(len(order)):
            if n + 1 < len(order):
                score(n + 1)
            weigh(n)

    def unit_at(d, odd):
        return up_by(u, (1 - 2 * odd) * MAJOR * d)

    def counts(unit):
        return (unit <= u) | ((core == 1) & (z_at > 0))

    def event(d, odd, i):
        unit = unit_at(d, odd)
        f = up_by(a, ORDER[i])
        early = 1 if i < RING // 2 else 0
        if odd:
            lands = goes = (core == 1) | (unit < FAR)
            to = major_to
        else:
            lands = (core == 1) | (unit < u)
            goes = (core == 1) | ((unit < u) & (u < RING - 1))
            to = minor_to
        onward = goes & ((d < NEAR) | ((d == NEAR) & (odd == jnp.where(shares(unit), early, 1))))

        @pl.when(lands & ((core == 0) | (f <= a)))
        def _():
            unit_copy(unit, f, me, 0).wait_recv()

            @pl.when(onward)
            def _():
                unit_copy(unit, f, to, 2 * d + 1 - odd).start()

    def weave(d, d_ready, sides):
        for g in range(4):
            for i in range(g * 2, (g + 1) * 2):
                for odd in sides:
                    event(d, odd, i)
            odd = 1 - g // 2
            unit = unit_at(d_ready, odd)
            part_of = range(g % 2 * 2, (g % 2 + 1) * 2)

            @pl.when(counts(unit) & ((d_ready > 0) | (odd == 1)))
            def _():
                absorb(unit, part_of, None)

    for i in range(1, ROW):
        slot = lax.rem(own_slot + i, ROW)
        q_copy(slot, own_slot, i).wait_recv()

    def stage(d, carry):
        weave(d, d - 1, (1, 0))
        return carry

    lax.fori_loop(1, NEAR + 1, stage, 0)
    def settle(n, carry):
        unit = unit_at(NEAR, 1 - n)

        @pl.when(counts(unit))
        def _():
            absorb(unit, range(ROW), None)

        return carry

    lax.fori_loop(0, 2, settle, 0)
    for i in range(RING):
        event(FAR, 1, i)
    last = unit_at(FAR, 1)
    valid = counts(last)

    def out_copy(slot, d, index):
        return pltpu.make_async_remote_copy(
            src_ref=out_send.at[d],
            dst_ref=out_recv.at[slot],
            send_sem=out_send_sem.at[index],
            recv_sem=out_recv_sem.at[slot],
            device_id=row_peer(d),
            device_id_type=MESH,
        )

    def stat_copy(slot, d, index):
        return pltpu.make_async_remote_copy(
            src_ref=stat_send.at[d],
            dst_ref=stat_recv.at[slot],
            send_sem=stat_send_sem.at[index],
            recv_sem=stat_recv_sem.at[slot],
            device_id=row_peer(d),
            device_id_type=MESH,
        )

    across = lax.rem(own_slot + 2, ROW)
    order = [across, across + 1 - 2 * core, own_slot + 1 - 2 * core, own_slot]

    def finish(n, total, top):
        for half in range(2):
            d = order[n] * 2 + half
            rows_of = slice(half * piece, (half + 1) * piece)
            weight = total[rows_of, width:]
            stat = top[rows_of] + math.log2(math.e) * jnp.log(weight)
            out_send[d] = (total[rows_of, :width] / weight).astype(jnp.bfloat16)
            stat_send[d] = stat.T[0:8]
            index = lax.rem(d - place + 8, 8)
            if n < ROW - 1:
                out_copy(place, d, index).start()
                stat_copy(place, d, index).start()
            else:

                @pl.when(d != place)
                def _():
                    out_copy(place, d, index).start()
                    stat_copy(place, d, index).start()

    @pl.when(valid)
    def _():
        absorb(last, order, finish)

    @pl.when(jnp.logical_not(valid))
    def _():
        for n in range(ROW):
            take = pl.ds(pl.multiple_of(order[n] * CH, CH), CH)
            finish(n, run_acc[take, :], run_max[take, :])

    keeps = [
        pltpu.make_async_copy(out_send.at[place], out_recv.at[place], store_sem.at[1]),
        pltpu.make_async_copy(stat_send.at[place], stat_recv.at[place], store_sem.at[2]),
    ]
    for copy in keeps:
        copy.start()

    out_order = (4, 5, 6, 7, 2, 3, 1)
    twin_copy(a, u, core).wait_send()
    for i in range(1, RING):

        @pl.when(spreads | (up_by(a, ORDER[i]) > a))
        def _():
            for half in range(2):
                first_copy(a, half, me, i).wait_send()

    for i in range(1, ROW):
        q_copy(own_slot, lax.rem(own_slot + i, ROW), i).wait_send()
    def drain(slot, carry):
        d = slot // 2
        odd = 1 - slot % 2
        unit = up_by(u, (1 - 2 * odd) * MAJOR * d)
        goes = (core == 1) | jnp.where(odd == 1, unit < FAR, (unit <= u) & (u < RING - 1))

        @pl.when(goes)
        def _():
            for i in range(RING):
                f = up_by(a, ORDER[i])
                early = 1 if i < RING // 2 else 0
                sent = (d < NEAR) | (odd == jnp.where(shares(unit), early, 1))

                @pl.when(sent & ((core == 0) | (f <= a)))
                def _():
                    unit_copy(u, f, me, slot).wait_send()

        return carry

    lax.fori_loop(0, RING, drain, 0)
    cache_store.wait()
    for i in out_order:
        slot = lax.rem(place + i, 8)
        out_copy(slot, place, i).wait_recv()
        stat_copy(slot, place, i).wait_recv()

    for i in out_order:
        out_copy(place, lax.rem(place + i, 8), i).wait_send()
        stat_copy(place, lax.rem(place + i, 8), i).wait_send()
    for copy in keeps:
        copy.wait()


def merge_kernel(heads, group, out_recv, stat_recv, cache_in, att, cache, wide_out):
    _, piece, width = out_recv.shape
    keep = piece // group
    cache[...] = cache_in[...]
    for core_from in range(2):
        for tp_from in range(2):
            low = core_from * 2 + tp_from
            wide_stat = [
                jnp.broadcast_to(stat_recv[s, 0:1, :], (piece, width)).T for s in (low, low + 4)
            ]
            gap = wide_stat[1] - wide_stat[0]
            merged = out_recv[low].astype(jnp.float32) / (1.0 + jnp.exp2(gap))
            merged = merged + out_recv[low + 4].astype(jnp.float32) / (1.0 + jnp.exp2(-gap))
            for g in range(group):
                head = tp_from * heads + core_from * group + g
                wide_out[pl.ds(head, keep, stride=2 * heads), :] = merged[g * keep : (g + 1) * keep]
    att[...] = wide_out[...].astype(jnp.bfloat16)


def build(ctx_size, queries, keys_in, values_in):
    rows, heads, width = queries.shape
    kv_heads = keys_in.shape[1]
    group = heads // kv_heads
    keep = rows // 2
    piece = group * keep
    fine, coarse = angle_tables(ctx_size, rows, width)
    f32, bf16 = jnp.float32, jnp.bfloat16

    hbm = pl.BlockSpec(memory_space=pl.ANY)
    dma = pltpu.SemaphoreType.DMA
    parts, stats, cache = pl.pallas_call(
        functools.partial(kernel, heads, kv_heads),
        out_shape=(
            jax.ShapeDtypeStruct((8, piece, width), bf16),
            jax.ShapeDtypeStruct((8, 8, piece), f32),
            jax.ShapeDtypeStruct((rows * kv_heads, width), bf16),
        ),
        in_specs=[hbm] * 5,
        out_specs=(hbm, hbm, hbm),
        scratch_shapes=[
            pltpu.VMEM((rows * heads, width), bf16),
            pltpu.VMEM((rows * kv_heads, width), bf16),
            pltpu.VMEM((rows * kv_heads, width), bf16),
            pltpu.VMEM((2, rows, width), f32),
            pltpu.VMEM((2, 8, width), f32),
            pltpu.VMEM((2, rows * kv_heads, width), f32),
            pltpu.VMEM((rows * heads, width), f32),
            pltpu.VMEM((kv_heads, 2, rows, width), bf16),
            pltpu.VMEM((RING, RING, 2, 2, rows, width), bf16),
            pltpu.VMEM((2, 2, group, keep, width), bf16),
            pltpu.VMEM((ROW, 2, group, keep, width), bf16),
            pltpu.VMEM((8 * piece, width), f32),
            pltpu.VMEM((8 * piece, 2 * width), f32),
            pltpu.VMEM((NB, CH, RING * 2 * rows), f32),
            pltpu.VMEM((8, piece, width), bf16),
            pltpu.VMEM((8, 8, piece), f32),
            pltpu.VMEM((rows * kv_heads, width), bf16),
            dma((5,)),
            dma((3,)),
            dma,
            dma,
            dma((2 * RING, 2)),
            dma((RING, 2)),
            dma((RING, RING)),
            dma((RING, RING)),
            dma((ROW,)),
            dma((ROW,)),
            dma((8,)),
            dma((8,)),
            dma((8,)),
            dma((8,)),
        ],
        compiler_params=pltpu.CompilerParams(collective_id=0, has_side_effects=True, vmem_limit_bytes=20 * 2**20),
    )(
        *(
            pltpu.with_memory_space_constraint(x, pltpu.HBM)
            for x in (
                queries.reshape(rows * heads, width),
                keys_in.reshape(rows * kv_heads, width),
                values_in.reshape(rows * kv_heads, width),
                jnp.asarray(fine),
                jnp.asarray(coarse),
            )
        )
    )
    vmem = pl.BlockSpec(memory_space=pltpu.VMEM)
    att, cache = pl.pallas_call(
        functools.partial(merge_kernel, heads, group),
        out_shape=(
            jax.ShapeDtypeStruct((2 * heads * keep, width), bf16),
            jax.ShapeDtypeStruct((rows * kv_heads, width), bf16),
        ),
        in_specs=[vmem] * 3,
        out_specs=(vmem, vmem),
        scratch_shapes=[pltpu.VMEM((2 * heads * keep, width), f32)],
        compiler_params=pltpu.CompilerParams(vmem_limit_bytes=8 * 2**20),
    )(parts, stats, cache)
    return att.reshape(keep, 2 * heads, width), cache.reshape(rows, kv_heads, width)


def solution(mesh):
    ctx_size = mesh.shape["ctx"]

    def per_device(queries, incoming_lookup_vectors, incoming_content_vectors):
        return build(ctx_size, queries, incoming_lookup_vectors, incoming_content_vectors)

    return jax.shard_map(
        per_device,
        mesh=mesh,
        in_specs=(P("ctx", "tp", None), P("ctx", "tp", None), P("ctx", "tp", None)),
        out_specs=(P(("ctx", "tp"), None, None), P("ctx", "tp", None)),
        check_vma=False,
    )
```

```python
import functools
import math

import jax
import jax.numpy as jnp
import numpy as np
from jax import lax
from jax.experimental import pallas as pl
from jax.experimental.pallas import tpu as pltpu
from jax.sharding import PartitionSpec as P

rope_base = 500000.0
MESH = pl.DeviceIdType.MESH
ROW = 4
RING = 8
ORDER = (0, 1, 7, 2, 6, 3, 5, 4)
MAJOR = -1
FAR, NEAR = 4, 3
NEVER = -1e30
CH, NB = 256, 2


def angle_tables(blocks, rows, width):
    half = width // 2
    freq = rope_base ** (-(np.arange(half, dtype=np.float64) * 2.0 / width))
    freq = np.concatenate([freq, freq])[None, :]
    fine = np.arange(rows, dtype=np.float64)[:, None] * freq
    coarse = np.arange(blocks, dtype=np.float64)[:, None] * rows * freq
    fine_table = np.stack([np.cos(fine), np.sin(fine)]).astype(np.float32)
    coarse_table = np.stack([np.cos(coarse), np.sin(coarse)], 1).astype(np.float32)
    coarse_table = np.broadcast_to(coarse_table[:, :, None, :], (blocks, 2, 8, width))
    return fine_table, np.ascontiguousarray(coarse_table)


def kernel(
    heads,
    kv_heads,
    q_hbm,
    k_hbm,
    v_hbm,
    fine_hbm,
    coarse_hbm,
    out_recv,
    stat_recv,
    cache_hbm,
    q_in,
    k_in,
    v_in,
    fine,
    coarse,
    wide_kv,
    wide_q,
    kv_own,
    kv,
    q_send,
    q_all,
    run_max,
    run_acc,
    score_buf,
    out_send,
    stat_send,
    cache_vmem,
    load_sem,
    store_sem,
    twin_send,
    twin_recv,
    first_send,
    first_recv,
    unit_send,
    unit_recv,
    q_send_sem,
    q_recv_sem,
    out_send_sem,
    out_recv_sem,
    stat_send_sem,
    stat_recv_sem,
):
    rows = k_in.shape[0] // kv_heads
    width = k_in.shape[1]
    half_width = width // 2
    group = heads // kv_heads
    keep = rows // 2
    span = 2 * rows
    piece = group * keep
    keys = RING * span
    me = lax.axis_index("ctx")
    part = lax.axis_index("tp")
    core = me % 2
    x_hi = (me // 2) % 2
    y_at = (me // ROW) % RING
    z_at = me // (ROW * RING)
    along_y = 1 - core
    a = along_y * y_at + core * z_at
    u = along_y * z_at + core * y_at
    first_stride = along_y * ROW + core * ROW * RING
    second_stride = along_y * ROW * RING + core * ROW
    row_base = me - me % ROW
    twin = me + 1 - 2 * core
    place = (me % ROW) * 2 + part

    def first_peer(f):
        return me + (f - a) * first_stride

    def second_peer(w):
        return me + (w - u) * second_stride

    def up_by(value, d):
        return lax.rem(value + d + RING, RING)

    def row_peer(d):
        return {"ctx": row_base + d // 2, "tp": d % 2}

    loads = [
        pltpu.make_async_copy(k_hbm, k_in, load_sem.at[0]),
        pltpu.make_async_copy(v_hbm, v_in, load_sem.at[1]),
        pltpu.make_async_copy(fine_hbm, fine, load_sem.at[2]),
        pltpu.make_async_copy(coarse_hbm.at[me], coarse, load_sem.at[3]),
        pltpu.make_async_copy(q_hbm, q_in, load_sem.at[4]),
    ]
    for load in loads:
        load.start()

    barrier = pltpu.get_barrier_semaphore()
    for d in range(1, RING):
        to = first_peer(up_by(a, d))
        pl.semaphore_signal(barrier, inc=1, device_id={"ctx": to}, device_id_type=MESH)
    for d in (1, -1):
        to = second_peer(up_by(u, d))
        pl.semaphore_signal(barrier, inc=1, device_id={"ctx": to}, device_id_type=MESH)
    for i in range(1, 8):
        to = row_peer(lax.rem(place + i, 8))
        pl.semaphore_signal(barrier, inc=1, device_id=to, device_id_type=MESH)


    loads[2].wait()
    loads[3].wait()
    cos_c = coarse[0, 0:1, :]
    sin_c = coarse[1, 0:1, :]
    cosine = cos_c * fine[0] - sin_c * fine[1]
    sine = sin_c * fine[0] + cos_c * fine[1]
    lane = lax.broadcasted_iota(jnp.int32, (rows, width), 1)
    sine = jnp.where(lane < half_width, -sine, sine)

    def turn(x):
        return x * cosine + pltpu.roll(x, half_width, 1) * sine

    loads[0].wait()
    loads[1].wait()
    wide_kv[0] = k_in[...].astype(jnp.float32)
    wide_kv[1] = v_in[...].astype(jnp.float32)
    for j in range(kv_heads):
        take = pl.ds(j, rows, stride=kv_heads)
        key_rot = turn(wide_kv[0, take, :])
        wide_kv[0, take, :] = key_rot
        kv_own[j, 0] = key_rot.astype(jnp.bfloat16)
        kv_own[j, 1] = wide_kv[1, take, :].astype(jnp.bfloat16)
    kv[u, a, core] = kv_own[core]
    pl.semaphore_wait(barrier, (RING - 1) + 2 + 7)

    def twin_copy(unit, f, half):
        return pltpu.make_async_remote_copy(
            src_ref=kv_own.at[1 - core],
            dst_ref=kv.at[unit, f, half],
            send_sem=twin_send,
            recv_sem=twin_recv,
            device_id={"ctx": twin},
            device_id_type=MESH,
        )

    def first_copy(f, half, to, slot):
        return pltpu.make_async_remote_copy(
            src_ref=kv.at[u, f, half],
            dst_ref=kv.at[u, f, half],
            send_sem=first_send.at[slot, half],
            recv_sem=first_recv.at[f, half],
            device_id={"ctx": to},
            device_id_type=MESH,
        )

    def unit_copy(unit, f, to, slot):
        return pltpu.make_async_remote_copy(
            src_ref=kv.at[unit, f],
            dst_ref=kv.at[unit, f],
            send_sem=unit_send.at[slot, f],
            recv_sem=unit_recv.at[unit, f],
            device_id={"ctx": to},
            device_id_type=MESH,
        )

    def q_copy(slot, to_slot, index):
        return pltpu.make_async_remote_copy(
            src_ref=q_send.at[to_slot % 2],
            dst_ref=q_all.at[slot],
            send_sem=q_send_sem.at[index],
            recv_sem=q_recv_sem.at[slot],
            device_id={"ctx": row_base + to_slot},
            device_id_type=MESH,
        )

    spreads = (core == 0) & (u < RING - 1)

    def climbs(unit):
        return (core == 1) | ((unit <= u) & (u < RING - 1))

    def wraps(unit):
        return (core == 1) | (unit < FAR)

    def spread(half, i_list):
        for i in i_list:
            to = up_by(a, ORDER[i])

            @pl.when(spreads | (to > a))
            def _():
                first_copy(a, half, first_peer(to), i).start()


    major_to = second_peer(up_by(u, MAJOR))
    minor_to = second_peer(up_by(u, -MAJOR))

    twin_copy(a, u, core).start()
    spread(core, (1, 2, 3, 4, 5, 6, 7))

    cache_vmem[...] = wide_kv[0].astype(jnp.bfloat16)
    cache_store = pltpu.make_async_copy(cache_vmem, cache_hbm, store_sem.at[0])
    cache_store.start()
    own_slot = me % ROW
    loads[4].wait()
    wide_q[...] = q_in[...].astype(jnp.float32)
    for h in range(heads):
        turned = turn(wide_q[pl.ds(h, rows, stride=heads), :]).astype(jnp.bfloat16)
        for half in range(2):
            q_send[h // group, half, h % group] = turned[half * keep : (half + 1) * keep]

    twin_copy(u, a, 1 - core).wait_recv()
    spread(1 - core, (1, 2, 3, 4, 5, 6, 7))
    pl.when(wraps(u))(lambda: unit_copy(u, a, major_to, 0).start())
    pl.when(climbs(u))(lambda: unit_copy(u, a, minor_to, 1).start())
    for i in range(1, ROW):
        q_copy(own_slot, lax.rem(own_slot + i, ROW), i).start()
    q_all[own_slot] = q_send[core]
    @pl.when((core == 0) & (u == RING - 1))
    def _():
        def clear(f, carry):
            kv[u, f] = jnp.zeros((2, 2, rows, width), jnp.bfloat16)
            return carry

        lax.fori_loop(a + 1, RING, clear, 0)

    @pl.when(core == 1)
    def _():
        def clear(f, carry):
            kv[:, f] = jnp.zeros((RING, 2, 2, rows, width), jnp.bfloat16)
            return carry

        lax.fori_loop(a + 1, RING, clear, 0)

    run_max[...] = jnp.full(run_max.shape, NEVER, jnp.float32)
    run_acc[...] = jnp.zeros(run_acc.shape, jnp.float32)

    def next_hop(i):
        return first_peer(up_by(a, 1 if ORDER[i] > RING // 2 else -1))

    def pass_on(f, half, i, slot):
        first_copy(f, half, next_hop(i), slot).start()
        first_sends.append((half, slot))

    def early(i):
        f = up_by(a, ORDER[i])
        for k, to in ((0, major_to), (1, minor_to)):
            unit = up_by(u, (2 * k - 1) * MAJOR)
            unit_copy(unit, f, me, 0).wait_recv()
            unit_copy(unit, f, to, 2 + k).start()

    for i in range(1, RING):
        f = up_by(a, ORDER[i])

        @pl.when(spreads | (f < a))
        def _():
            for half in range(2):
                first_copy(f, half, me, i).wait_recv()

            @pl.when(wraps(u))
            def _():
                unit_copy(u, f, major_to, 0).start()

            @pl.when(climbs(u))
            def _():
                unit_copy(u, f, minor_to, 1).start()

    factor = math.log2(math.e) / math.sqrt(width)
    unit_step = along_y * (span * 2 * RING) + core * span * 2
    block_step = along_y * span * 2 + core * (span * 2 * RING)
    row_start = (z_at * RING + y_at) * span * 2

    def absorb(unit, order, done):
        key_block = kv[unit, :, :, 0].reshape(keys, width)
        value_block = kv[unit, :, :, 1].reshape(keys, width)
        extended = jnp.concatenate([value_block, jnp.ones_like(value_block)], axis=1)
        col = lax.broadcasted_iota(jnp.int32, (1, keys), 1)
        k_at = unit * unit_step + (col // span) * block_step + x_hi * span + col % span - row_start
        at = lax.broadcasted_iota(jnp.int32, (CH, 1), 0)

        def score(n):
            r = order[n]
            scores = factor * lax.dot_general(
                q_all[r].reshape(CH, width),
                key_block,
                (((1,), (1,)), ((), ())),
                preferred_element_type=jnp.float32,
            )
            q_at = (2 * r + at // piece) * keep + at % keep
            score_buf[n % NB] = jnp.where(k_at <= q_at, scores, NEVER)

        def weigh(n):
            take = pl.ds(pl.multiple_of(order[n] * CH, CH), CH)
            old = run_max[take, 0:1]
            top = jnp.maximum(old, jnp.max(score_buf[n % NB], axis=1, keepdims=True))
            weights = jnp.exp2(score_buf[n % NB] - top).astype(jnp.bfloat16)
            total = jnp.dot(weights, extended, preferred_element_type=jnp.float32)
            total = total + jnp.exp2(old - top) * run_acc[take, :]
            top = jnp.broadcast_to(top, (CH, width))
            if done is None:
                run_acc[take, :] = total
                run_max[take, :] = top
            else:
                done(n, total, top)

        score(0)
        for n in range(len(order)):
            if n + 1 < len(order):
                score(n + 1)
            weigh(n)

    def unit_at(d, odd):
        return up_by(u, (1 - 2 * odd) * MAJOR * d)

    def counts(unit):
        return (unit <= u) | ((core == 1) & (z_at > 0))

    def event(d, odd, i):
        unit = unit_at(d, odd)
        f = up_by(a, ORDER[i])
        early = 1 if i < RING // 2 else 0
        if odd:
            lands = goes = (core == 1) | (unit < FAR)
            to = major_to
        else:
            lands = (core == 1) | (unit < u)
            goes = (core == 1) | ((unit < u) & (u < RING - 1))
            to = minor_to
        onward = goes & ((d < NEAR) | ((d == NEAR) & (odd == early)))

        @pl.when(lands & ((core == 0) | (f <= a)))
        def _():
            unit_copy(unit, f, me, 0).wait_recv()

            @pl.when(onward)
            def _():
                unit_copy(unit, f, to, 2 * d + 1 - odd).start()

    def weave(d, d_ready, sides):
        for g in range(4):
            odd = 1 - g // 2
            unit = unit_at(d_ready, odd)
            part_of = range(g % 2 * 2, (g % 2 + 1) * 2)

            @pl.when(counts(unit) & ((d_ready > 0) | (odd == 1)))
            def _():
                absorb(unit, part_of, None)

            for i in range(g * 2, (g + 1) * 2):
                for odd in sides:
                    event(d, odd, i)

    for i in range(1, ROW):
        slot = lax.rem(own_slot + i, ROW)
        q_copy(slot, own_slot, i).wait_recv()

    def stage(d, carry):
        weave(d, d - 1, (1, 0))
        return carry

    lax.fori_loop(1, NEAR + 1, stage, 0)
    def settle(n, carry):
        unit = unit_at(NEAR, 1 - n)

        @pl.when(counts(unit))
        def _():
            absorb(unit, range(ROW), None)

        return carry

    lax.fori_loop(0, 2, settle, 0)
    for i in range(RING):
        event(FAR, 1, i)
    last = unit_at(FAR, 1)
    valid = counts(last)

    def out_copy(slot, d, index):
        return pltpu.make_async_remote_copy(
            src_ref=out_send.at[d],
            dst_ref=out_recv.at[slot],
            send_sem=out_send_sem.at[index],
            recv_sem=out_recv_sem.at[slot],
            device_id=row_peer(d),
            device_id_type=MESH,
        )

    def stat_copy(slot, d, index):
        return pltpu.make_async_remote_copy(
            src_ref=stat_send.at[d],
            dst_ref=stat_recv.at[slot],
            send_sem=stat_send_sem.at[index],
            recv_sem=stat_recv_sem.at[slot],
            device_id=row_peer(d),
            device_id_type=MESH,
        )

    across = lax.rem(own_slot + 2, ROW)
    order = [across, across + 1 - 2 * core, own_slot + 1 - 2 * core, own_slot]

    def finish(n, total, top):
        for half in range(2):
            d = order[n] * 2 + half
            rows_of = slice(half * piece, (half + 1) * piece)
            weight = total[rows_of, width:]
            stat = top[rows_of] + math.log2(math.e) * jnp.log(weight)
            out_send[d] = (total[rows_of, :width] / weight).astype(jnp.bfloat16)
            stat_send[d] = stat.T[0:8]
            index = lax.rem(d - place + 8, 8)
            if n < ROW - 1:
                out_copy(place, d, index).start()
                stat_copy(place, d, index).start()
            else:

                @pl.when(d != place)
                def _():
                    out_copy(place, d, index).start()
                    stat_copy(place, d, index).start()

    @pl.when(valid)
    def _():
        absorb(last, order, finish)

    @pl.when(jnp.logical_not(valid))
    def _():
        for n in range(ROW):
            take = pl.ds(pl.multiple_of(order[n] * CH, CH), CH)
            finish(n, run_acc[take, :], run_max[take, :])

    keeps = [
        pltpu.make_async_copy(out_send.at[place], out_recv.at[place], store_sem.at[1]),
        pltpu.make_async_copy(stat_send.at[place], stat_recv.at[place], store_sem.at[2]),
    ]
    for copy in keeps:
        copy.start()

    out_order = (4, 5, 6, 7, 2, 3, 1)
    twin_copy(a, u, core).wait_send()
    for i in range(1, RING):

        @pl.when(spreads | (up_by(a, ORDER[i]) > a))
        def _():
            for half in range(2):
                first_copy(a, half, me, i).wait_send()

    for i in range(1, ROW):
        q_copy(own_slot, lax.rem(own_slot + i, ROW), i).wait_send()
    def drain(slot, carry):
        d = slot // 2
        odd = 1 - slot % 2
        unit = up_by(u, (1 - 2 * odd) * MAJOR * d)
        goes = (core == 1) | jnp.where(odd == 1, unit < FAR, (unit <= u) & (u < RING - 1))

        @pl.when(goes)
        def _():
            for i in range(RING):
                f = up_by(a, ORDER[i])
                early = 1 if i < RING // 2 else 0
                sent = (d < NEAR) | (odd == early)

                @pl.when(sent & ((core == 0) | (f <= a)))
                def _():
                    unit_copy(u, f, me, slot).wait_send()

        return carry

    lax.fori_loop(0, RING, drain, 0)
    cache_store.wait()
    for i in out_order:
        slot = lax.rem(place + i, 8)
        out_copy(slot, place, i).wait_recv()
        stat_copy(slot, place, i).wait_recv()

    for i in out_order:
        out_copy(place, lax.rem(place + i, 8), i).wait_send()
        stat_copy(place, lax.rem(place + i, 8), i).wait_send()
    for copy in keeps:
        copy.wait()


def merge_kernel(heads, group, out_recv, stat_recv, cache_in, att, cache, wide_out):
    _, piece, width = out_recv.shape
    keep = piece // group
    cache[...] = cache_in[...]
    for core_from in range(2):
        for tp_from in range(2):
            low = core_from * 2 + tp_from
            wide_stat = [
                jnp.broadcast_to(stat_recv[s, 0:1, :], (piece, width)).T for s in (low, low + 4)
            ]
            gap = wide_stat[1] - wide_stat[0]
            merged = out_recv[low].astype(jnp.float32) / (1.0 + jnp.exp2(gap))
            merged = merged + out_recv[low + 4].astype(jnp.float32) / (1.0 + jnp.exp2(-gap))
            for g in range(group):
                head = tp_from * heads + core_from * group + g
                wide_out[pl.ds(head, keep, stride=2 * heads), :] = merged[g * keep : (g + 1) * keep]
    att[...] = wide_out[...].astype(jnp.bfloat16)


def build(ctx_size, queries, keys_in, values_in):
    rows, heads, width = queries.shape
    kv_heads = keys_in.shape[1]
    group = heads // kv_heads
    keep = rows // 2
    piece = group * keep
    fine, coarse = angle_tables(ctx_size, rows, width)
    f32, bf16 = jnp.float32, jnp.bfloat16

    hbm = pl.BlockSpec(memory_space=pl.ANY)
    dma = pltpu.SemaphoreType.DMA
    parts, stats, cache = pl.pallas_call(
        functools.partial(kernel, heads, kv_heads),
        out_shape=(
            jax.ShapeDtypeStruct((8, piece, width), bf16),
            jax.ShapeDtypeStruct((8, 8, piece), f32),
            jax.ShapeDtypeStruct((rows * kv_heads, width), bf16),
        ),
        in_specs=[hbm] * 5,
        out_specs=(hbm, hbm, hbm),
        scratch_shapes=[
            pltpu.VMEM((rows * heads, width), bf16),
            pltpu.VMEM((rows * kv_heads, width), bf16),
            pltpu.VMEM((rows * kv_heads, width), bf16),
            pltpu.VMEM((2, rows, width), f32),
            pltpu.VMEM((2, 8, width), f32),
            pltpu.VMEM((2, rows * kv_heads, width), f32),
            pltpu.VMEM((rows * heads, width), f32),
            pltpu.VMEM((kv_heads, 2, rows, width), bf16),
            pltpu.VMEM((RING, RING, 2, 2, rows, width), bf16),
            pltpu.VMEM((2, 2, group, keep, width), bf16),
            pltpu.VMEM((ROW, 2, group, keep, width), bf16),
            pltpu.VMEM((8 * piece, width), f32),
            pltpu.VMEM((8 * piece, 2 * width), f32),
            pltpu.VMEM((NB, CH, RING * 2 * rows), f32),
            pltpu.VMEM((8, piece, width), bf16),
            pltpu.VMEM((8, 8, piece), f32),
            pltpu.VMEM((rows * kv_heads, width), bf16),
            dma((5,)),
            dma((3,)),
            dma,
            dma,
            dma((2 * RING, 2)),
            dma((RING, 2)),
            dma((RING, RING)),
            dma((RING, RING)),
            dma((ROW,)),
            dma((ROW,)),
            dma((8,)),
            dma((8,)),
            dma((8,)),
            dma((8,)),
        ],
        compiler_params=pltpu.CompilerParams(collective_id=0, has_side_effects=True, vmem_limit_bytes=20 * 2**20),
    )(
        *(
            pltpu.with_memory_space_constraint(x, pltpu.HBM)
            for x in (
                queries.reshape(rows * heads, width),
                keys_in.reshape(rows * kv_heads, width),
                values_in.reshape(rows * kv_heads, width),
                jnp.asarray(fine),
                jnp.asarray(coarse),
            )
        )
    )
    vmem = pl.BlockSpec(memory_space=pltpu.VMEM)
    att, cache = pl.pallas_call(
        functools.partial(merge_kernel, heads, group),
        out_shape=(
            jax.ShapeDtypeStruct((2 * heads * keep, width), bf16),
            jax.ShapeDtypeStruct((rows * kv_heads, width), bf16),
        ),
        in_specs=[vmem] * 3,
        out_specs=(vmem, vmem),
        scratch_shapes=[pltpu.VMEM((2 * heads * keep, width), f32)],
        compiler_params=pltpu.CompilerParams(vmem_limit_bytes=8 * 2**20),
    )(parts, stats, cache)
    return att.reshape(keep, 2 * heads, width), cache.reshape(rows, kv_heads, width)


def solution(mesh):
    ctx_size = mesh.shape["ctx"]

    def per_device(queries, incoming_lookup_vectors, incoming_content_vectors):
        return build(ctx_size, queries, incoming_lookup_vectors, incoming_content_vectors)

    return jax.shard_map(
        per_device,
        mesh=mesh,
        in_specs=(P("ctx", "tp", None), P("ctx", "tp", None), P("ctx", "tp", None)),
        out_specs=(P(("ctx", "tp"), None, None), P("ctx", "tp", None)),
        check_vma=False,
    )
```
